32 devices in a mesh: member: 2 (over y), tile: 4 (over z), lev: 2 (over x), sub: 2 (over core).
Axes of the slice: x: 2, y: 2, z: 4, core: 2. Of those that a mesh axis runs over, the one named last changes fastest.
Arguments:
- increment: float32 [4, 1024, 128], P(('member', 'lev'), ('tile', 'sub')), parts along dimension 0, may hold values from -6 to 6
- residual: float32 [4, 1024, 128], P(('member', 'lev'), ('tile', 'sub')), parts along dimension 0, may hold values from -6 to 6
- direction: float32 [4, 1024, 128], P(('member', 'lev'), ('tile', 'sub')), parts along dimension 0, may hold values from -6 to 6
- wind_u: bfloat16 [4, 1024, 128], P(('member', 'lev'), ('tile', 'sub')), parts along dimension 0, may hold values from -0.3984375 to 0.3984375
- wind_v: bfloat16 [4, 1024, 128], P(('member', 'lev'), ('tile', 'sub')), parts along dimension 0, may hold values from -0.3984375 to 0.3984375
- diffusion: float32 [2], replicated, may hold values from 0.03 to 0.12
- vertical: float32 [2], replicated, may hold values from 0.02 to 0.1
- background_inv: float32 [2], replicated, may hold values from 0.5 to 2
- side_pair: int32 [8, 4], replicated, may hold values from 0 to 31, as said below
- side_flip: int32 [8, 4], replicated, may hold values from 0 to 1, as said below
- obs_column: int32 [512], P(('tile', 'sub')), may hold values from 0 to 131071, as said below
- obs_time: int32 [512], P(('tile', 'sub')), may hold values from 1 to 4
- obs_count: int32 [8], P(('tile', 'sub')), may hold values from 48 to 64, as said below
- jacobian: bfloat16 [512, 2, 616], P(('tile', 'sub'), 'lev'), may hold values from -4 to 4
- error_inv: float32 [616], replicated, may hold values from 0.2 to 5
Outputs:
- increment_new: float32 [4, 1024, 128], P(('member', 'lev'), ('tile', 'sub')), parts along dimension 0
- residual_new: float32 [4, 1024, 128], P(('member', 'lev'), ('tile', 'sub')), parts along dimension 0
- direction_new: float32 [4, 1024, 128], P(('member', 'lev'), ('tile', 'sub')), parts along dimension 0
The draws below stay inside these ranges and needn't reach their ends.
There are 2 independent parts, one for each index of `member`. The reference program is written for one: setup_inputs(seed, part) draws one part's arguments, and reference() takes and returns one part's arrays. A program takes and returns all parts, laid end to end along the dimension named above; an argument that names none is the same for every part. Nothing has to cross between parts.
Inputs may be any that keep to these rules, and one draw needn't show every extreme that they name: side_pair[side_pair[k]] == k for every side k, and side_pair[k] is a side of another panel, so the panels close into one surface joined edge to edge. side_flip is equal on both sides of a pair. `obs_column`: among the live slots of one owner at most 16 name columns of one panel, and every owner reaches 16 for some panel. `obs_count`: some owner has all 64 slots live.
All inputs are finite; a program needn't handle non-finite values.
Results may differ from the reference program's by a relative error of at most 0.0003.
Values sent between devices are 32-bit elements; how exact they have to be, the bound alone decides.
No kernel may reach another device: no remote copies, remote signals or barrier semaphores. Data moves between devices by JAX's collectives and lax.ppermute only.
A program may use at most 64 MiB of HBM per device.

```python
import math
import jax
import jax.numpy as jnp
from jax import lax

W = 128
STEPS = 4
CH = 616
OBS_DEV = 64
PANELS = 8
LEVELS = 2
NOBS = 512
CAP = 16


def side_pairing(key):
    inner = jax.random.fold_in(key, 7)
    first_key, second_key = jax.random.split(inner)
    order = jax.random.permutation(first_key, PANELS).astype(jnp.int32)
    stride = 1 + PANELS // 8
    places = jnp.arange(PANELS, dtype=jnp.int32)
    below = order[(places + 1) % PANELS]
    beside = order[(places + stride) % PANELS]
    lower_sides = 4 * order + 1
    upper_sides = 4 * below + 0
    east_sides = 4 * order + 3
    west_sides = 4 * beside + 2
    leading = jnp.concatenate([lower_sides, east_sides]).astype(jnp.int32)
    trailing = jnp.concatenate([upper_sides, west_sides]).astype(jnp.int32)
    paired = jnp.zeros((4 * PANELS,), jnp.int32).at[leading].set(trailing).at[trailing].set(leading)
    bits = jax.random.randint(second_key, (2 * PANELS,), 0, 2).astype(jnp.int32)
    flipped = jnp.zeros((4 * PANELS,), jnp.int32).at[leading].set(bits).at[trailing].set(bits)
    return (paired.reshape(PANELS, 4), flipped.reshape(PANELS, 4))


def draw_side_pair(key, part):
    return side_pairing(key)[0]


def draw_side_flip(key, part):
    return side_pairing(key)[1]


def draw_obs_column(key, part):
    inner = jax.random.fold_in(key, 11)

    def one_owner(owner_key):
        perm_key, shuffle_key, cell_key = jax.random.split(owner_key, 3)
        order = jax.random.permutation(perm_key, PANELS).astype(jnp.int32)
        others = jax.random.permutation(shuffle_key, jnp.repeat(order[1:], CAP))
        targets = jnp.concatenate([jnp.full((CAP,), order[0], jnp.int32), others.astype(jnp.int32)])[:OBS_DEV]
        cells = jax.random.randint(cell_key, (OBS_DEV,), 0, W * W).astype(jnp.int32)
        return targets * (W * W) + cells
    return jax.vmap(one_owner)(jax.random.split(inner, PANELS)).reshape(PANELS * OBS_DEV).astype(jnp.int32)


def draw_obs_count(key, part):
    inner = jax.random.fold_in(key, 13)
    count_key, pick_key = jax.random.split(inner)
    counts = jax.random.randint(count_key, (PANELS,), (3 * OBS_DEV + 3) // 4, OBS_DEV + 1).astype(jnp.int32)
    chosen = jax.random.randint(pick_key, (), 0, PANELS)
    return counts.at[chosen].set(OBS_DEV)


def set_ends(result, key, smallest, high):
    dims = result.shape
    place = [jax.random.randint(jax.random.fold_in(key, axis), (), 0, dims[axis]) for axis in range(len(dims))]
    result = result.at[tuple(place)].set(smallest)
    longest = dims.index(max(dims))
    place[longest] = (place[longest] + 1) % dims[longest]
    return result.at[tuple(place)].set(high)


def level_of(stream_key, extent, cuts, smallest, top_value):
    def one(position, shards_of):
        steps = jax.random.uniform(jax.random.fold_in(jax.random.fold_in(stream_key, 6), position), (shards_of,), jnp.float32, smallest / len(cuts), top_value / len(cuts))
        return jnp.repeat(jnp.exp(steps), extent[position] // shards_of).reshape((-1,) + (1,) * (len(extent) - position - 1))

    factor_of = one(*cuts[0])
    for cut in cuts[1:]:
        factor_of = factor_of * one(*cut)
    return factor_of


def scatter_about(key, extent, scale, bound, pieces=(), held_as=jnp.bfloat16):
    entries = scale * jax.random.normal(key, extent, jnp.float32)
    if pieces:
        entries = entries * level_of(key, extent, pieces, -0.22, 0.18)
    return jnp.clip(entries, -bound, bound).astype(held_as)


def setup_inputs(seed: int = 0, part: int = 0) -> dict:
    key_list = jax.random.split(jax.random.key(seed), 16)
    part_keys = jax.random.split(jax.random.fold_in(key_list[15], part), 16)
    return {
        "increment": scatter_about(part_keys[0], (LEVELS, PANELS * W, W), 1.0, 6.0, ((0, 2), (1, 8)), jnp.float32),
        "residual": scatter_about(part_keys[1], (LEVELS, PANELS * W, W), 1.0, 6.0, ((0, 2), (1, 8)), jnp.float32),
        "direction": scatter_about(part_keys[2], (LEVELS, PANELS * W, W), 1.0, 6.0, ((0, 2), (1, 8)), jnp.float32),
        "wind_u": jnp.clip(jax.random.uniform(part_keys[3], (LEVELS, PANELS * W, W), jnp.float32, -0.3984375, 0.3984375) * level_of(part_keys[3], (LEVELS, PANELS * W, W), ((0, 2), (1, 8)), -0.4, 0.0), -0.3984375, 0.3984375).astype(jnp.bfloat16),
        "wind_v": jnp.clip(jax.random.uniform(part_keys[4], (LEVELS, PANELS * W, W), jnp.float32, -0.3984375, 0.3984375) * level_of(part_keys[4], (LEVELS, PANELS * W, W), ((0, 2), (1, 8)), -0.4, 0.0), -0.3984375, 0.3984375).astype(jnp.bfloat16),
        "diffusion": jnp.clip(jnp.exp(jax.random.uniform(key_list[5], (LEVELS,), jnp.float32, math.log(0.03), math.log(0.12))), 0.03, 0.12),
        "vertical": jnp.clip(jnp.exp(jax.random.uniform(key_list[6], (LEVELS,), jnp.float32, math.log(0.02), math.log(0.1))), 0.02, 0.1),
        "background_inv": jnp.clip(jnp.exp(jax.random.uniform(key_list[7], (LEVELS,), jnp.float32, math.log(0.5), math.log(2.0))), 0.5, 2.0),
        "side_pair": draw_side_pair(jax.random.fold_in(key_list[15], 71), part),
        "side_flip": draw_side_flip(jax.random.fold_in(key_list[15], 71), part),
        "obs_column": draw_obs_column(jax.random.fold_in(key_list[15], 71), part),
        "obs_time": set_ends(jax.random.randint(key_list[11], (NOBS,), 1, STEPS + 1), jax.random.fold_in(key_list[11], 1), 1, STEPS).astype(jnp.int32),
        "obs_count": draw_obs_count(jax.random.fold_in(key_list[15], 71), part),
        "jacobian": scatter_about(key_list[13], (NOBS, LEVELS, CH), LEVELS ** -0.5, 4.0, ((0, 8), (1, 2))),
        "error_inv": jnp.clip(jnp.exp(jax.random.uniform(key_list[14], (CH,), jnp.float32, math.log(0.2), math.log(5.0))), 0.2, 5.0),
    }


def edge_strips(field):
    stacked = jnp.stack([field[:, :, 0, :], field[:, :, -1, :], field[:, :, :, 0], field[:, :, :, -1]], axis=0)
    return jnp.transpose(stacked, (2, 0, 1, 3)).reshape(PANELS * 4, LEVELS, W)


def neighbour_strips(strips, side_pair, side_flip):
    picked = strips[side_pair]
    picked = jnp.where(side_flip[:, :, None, None] == 1, picked[:, :, :, ::-1], picked)
    return jnp.transpose(picked, (1, 2, 0, 3))


def coefficients(wind_u, wind_v, diffusion, vertical):
    speed_u = wind_u.astype(jnp.float32).reshape(LEVELS, PANELS, W, W)
    speed_v = wind_v.astype(jnp.float32).reshape(LEVELS, PANELS, W, W)
    mixing = diffusion[:, None, None, None]
    coefs = (mixing + 0.5 * speed_u, mixing - 0.5 * speed_u, mixing + 0.5 * speed_v, mixing - 0.5 * speed_v)
    center = (1.0 - 4.0 * diffusion - 2.0 * vertical)[:, None, None, None]
    return coefs, center


def forward_step(field, coefs, center, vertical, side_pair, side_flip):
    halos = neighbour_strips(edge_strips(field), side_pair, side_flip)
    north = jnp.concatenate([halos[0][:, :, None, :], field[:, :, :-1, :]], axis=2)
    south = jnp.concatenate([field[:, :, 1:, :], halos[1][:, :, None, :]], axis=2)
    west = jnp.concatenate([halos[2][:, :, :, None], field[:, :, :, :-1]], axis=3)
    east = jnp.concatenate([field[:, :, :, 1:], halos[3][:, :, :, None]], axis=3)
    padded = jnp.pad(field, ((1, 1), (0, 0), (0, 0), (0, 0)))
    mixing = vertical[:, None, None, None] * (padded[:-2] + padded[2:])
    return center * field + coefs[0] * north + coefs[1] * south + coefs[2] * west + coefs[3] * east + mixing


def adjoint_step(field, coefs, center, vertical, side_pair, side_flip):
    prods = [c * field for c in coefs]
    strips = jnp.stack([prods[0][:, :, 0, :], prods[1][:, :, -1, :], prods[2][:, :, :, 0], prods[3][:, :, :, -1]], axis=0)
    strips = jnp.transpose(strips, (2, 0, 1, 3)).reshape(PANELS * 4, LEVELS, W)
    halos = neighbour_strips(strips, side_pair, side_flip)
    rows_term = jnp.concatenate([prods[0][:, :, 1:, :], halos[1][:, :, None, :]], axis=2)
    rows_term = rows_term + jnp.concatenate([halos[0][:, :, None, :], prods[1][:, :, :-1, :]], axis=2)
    cols_term = jnp.concatenate([prods[2][:, :, :, 1:], halos[3][:, :, :, None]], axis=3)
    cols_term = cols_term + jnp.concatenate([halos[2][:, :, :, None], prods[3][:, :, :, :-1]], axis=3)
    padded = jnp.pad(vertical[:, None, None, None] * field, ((1, 1), (0, 0), (0, 0), (0, 0)))
    return center * field + rows_term + cols_term + padded[:-2] + padded[2:]


def reference(increment, residual, direction, wind_u, wind_v, diffusion, vertical, background_inv, side_pair, side_flip, obs_column, obs_time, obs_count, jacobian, error_inv):
    coefs, center = coefficients(wind_u, wind_v, diffusion, vertical)
    state = direction.reshape(LEVELS, PANELS, W, W)
    states = []
    for step in range(STEPS):
        state = forward_step(state, coefs, center, vertical, side_pair, side_flip)
        states.append(state.reshape(LEVELS, PANELS * W * W))
    history = jnp.stack(states, axis=0)
    earlier = (obs_time - 1).astype(jnp.int32)
    columns = history[earlier, :, obs_column]
    live = (jnp.arange(OBS_DEV, dtype=jnp.int32)[None, :] < obs_count[:, None]).reshape(NOBS)
    live = live.astype(jnp.float32)

    def owner_block(items):
        block, values, alive = items
        wide = block.astype(jnp.float32)
        departure = jnp.einsum("olc,ol->oc", wide, values, precision=lax.Precision.HIGHEST)
        weighted = departure * error_inv[None, :]
        back = jnp.einsum("olc,oc->ol", wide, weighted, precision=lax.Precision.HIGHEST)
        return back * alive[:, None]

    adjoint_obs = lax.map(owner_block, (jacobian.reshape(PANELS, OBS_DEV, LEVELS, CH), columns.reshape(PANELS, OBS_DEV, LEVELS), live.reshape(PANELS, OBS_DEV)))
    adjoint_obs = adjoint_obs.reshape(NOBS, LEVELS)
    forcing = jnp.zeros((STEPS, LEVELS, PANELS * W * W), jnp.float32).at[earlier, :, obs_column].add(adjoint_obs)
    forcing = forcing.reshape(STEPS, LEVELS, PANELS, W, W)
    adjoint = forcing[STEPS - 1]
    for step in range(STEPS - 1, 0, -1):
        adjoint = adjoint_step(adjoint, coefs, center, vertical, side_pair, side_flip) + forcing[step - 1]
    adjoint = adjoint_step(adjoint, coefs, center, vertical, side_pair, side_flip)
    image = background_inv[:, None, None] * direction + adjoint.reshape(LEVELS, PANELS * W, W)
    norm_old = jnp.sum(residual * residual)
    alpha = norm_old / jnp.sum(direction * image)
    increment_new = increment + alpha * direction
    residual_new = residual - alpha * image
    norm_new = jnp.sum(residual_new * residual_new)
    direction_new = residual_new + (norm_new / norm_old) * direction
    return increment_new, residual_new, direction_new
```

```python
import jax
import jax.numpy as jnp
from jax import lax
from jax.experimental import pallas as pl
from jax.experimental.pallas import tpu as pltpu
from jax.sharding import PartitionSpec as P

STEPS = 4
DEEP = 2 * STEPS
SIDES = 4
FIELDS = 3
BAND = SIDES * FIELDS * DEEP
LANES = 128
SHEETS = LANES // DEEP
CHUNK = 512
F32 = jnp.float32
BF16 = jnp.bfloat16
NT = (((1,), (1,)), ((), ()))
WHOLE = pl.BlockSpec(memory_space=pltpu.VMEM)
SCALAR = pl.BlockSpec(memory_space=pltpu.SMEM)
CORNERS = ((0, 2), (0, 3), (1, 2), (1, 3))
NW, NE, SW, SE = range(4)


def iota(shape, axis):
    return lax.broadcasted_iota(jnp.int32, shape, axis)


def level_pairs(levels):
    return [(low, high) for low in range(levels) for high in range(low, levels)]


def record_rows(levels):
    return -(-(4 + len(level_pairs(levels))) // 8) * 8


def rotated(levels, k):
    return lax.rem(lax.axis_index("lev") + (levels - k), levels)


def prepare(direction, wind_u, wind_v, jacobian, bands, winds, wide):
    x = direction[...]
    u = 0.5 * wind_u[...].astype(F32)
    v = 0.5 * wind_v[...].astype(F32)
    width = x.shape[0]
    winds[0] = u
    winds[1] = v
    wide[...] = jacobian[...].astype(F32)
    first = lambda a: a[:DEEP]
    last = lambda a: jnp.concatenate([a[width - 1 - d : width - d] for d in range(DEEP)], axis=0)
    xt, ut, vt = x.T, u.T, v.T
    parts = [
        (first(x), first(u), first(v)),
        (last(x), -last(u), last(v)),
        (first(xt), first(vt), first(ut)),
        (last(xt), -last(vt), last(ut)),
    ]
    for side in range(SIDES):
        for field in range(FIELDS):
            row = (side * FIELDS + field) * DEEP
            bands[row : row + DEEP, :] = parts[side][field]


def compose(levels, *refs):
    bands = refs[:levels]
    jacobians = refs[levels : 2 * levels]
    error_inv, places, message, ordered = refs[2 * levels :]
    for k in range(levels):
        level = rotated(levels, k)
        message[pl.ds(pl.multiple_of(level * BAND, 8), BAND), :] = bands[k][...]
        ordered[level] = jacobians[k][...].astype(F32)
    slots = ordered.shape[1]
    base = levels * BAND
    place = places[...]
    ones = jnp.ones((8, ordered.shape[2]), F32)
    weights = error_inv[...]
    pairs = level_pairs(levels)
    rows = [place[:4, :]]
    for low, high in pairs:
        product = ordered[low] * weights * ordered[high]
        total = lax.dot_general(ones, product, NT, precision=lax.Precision.HIGHEST, preferred_element_type=F32)
        row = total[:1]
        if slots < LANES:
            row = jnp.concatenate([row, jnp.zeros((1, LANES - slots), F32)], axis=1)
        rows.append(row)
    spare = record_rows(levels) - 4 - len(pairs)
    if spare:
        rows.append(jnp.zeros((spare, LANES), F32))
    message[base : base + record_rows(levels), :] = jnp.concatenate(rows, axis=0)


def roll(a, shift, axis):
    return pltpu.roll(a, shift % a.shape[axis], axis)


class Geometry:
    def __init__(self, width):
        last = width - 1
        self.last = last
        row, lane = iota((width, LANES), 0), iota((width, LANES), 1)
        self.top, self.bottom = row == 0, row == last
        self.left, self.right = lane == 0, lane == last
        self.half = lane == LANES // 2
        brow, blane = iota((DEEP, LANES), 0), iota((DEEP, LANES), 1)
        self.band_first = brow == 0
        self.band_left, self.band_right = blane == 0, blane == last
        crow, clane = iota((SIDES * DEEP, LANES), 0), iota((SIDES * DEEP, LANES), 1)
        self.chain_top = crow % DEEP == 0
        self.chain_left = clane % DEEP == 0
        self.even = (clane // DEEP) % 2 == 0
        self.seventh = clane // DEEP == DEEP - 1
        self.near = iota((1, LANES), 1) < LANES // 2

    def chain(self, a, corner):
        return a[corner * DEEP : (corner + 1) * DEEP]

    def main_up(self, a, north):
        return jnp.where(self.top, north[:1], roll(a, 1, 0))

    def main_down(self, a, south):
        return jnp.where(self.bottom, south[:1], roll(a, -1, 0))

    def main_west(self, a, ew):
        return jnp.where(self.left, roll(ew, LANES // 2, 1), roll(a, 1, 1))

    def main_east(self, a, ew):
        return jnp.where(self.right, roll(ew, -1, 1), roll(a, -1, 1))

    def band_toward(self, a, main_row):
        return jnp.where(self.band_first, main_row, roll(a, 1, 0))

    def band_west(self, a, chain_block):
        return jnp.where(self.band_left, roll(chain_block, -2 * DEEP, 1), roll(a, 1, 1))

    def band_east(self, a, chain_block):
        return jnp.where(self.band_right, roll(chain_block, self.last - 2 * DEEP, 1), roll(a, -1, 1))

    def ew_toward(self, a, main_east, main_west):
        inner = jnp.where(self.half, roll(main_west, LANES // 2, 1), roll(a, 1, 1))
        return jnp.where(self.left, roll(main_east, 1, 1), inner)

    def ew_fill(self, east, west):
        return jnp.where(self.near, roll(east, 2 * DEEP, 1)[:1], roll(west, 2 * DEEP + LANES // 2, 1)[:1])

    def ew_up(self, a, chain):
        fill = self.ew_fill(self.chain(chain, NE), self.chain(chain, NW))
        return jnp.where(self.top, fill, roll(a, 1, 0))

    def ew_down(self, a, chain):
        fill = self.ew_fill(self.chain(chain, SE), self.chain(chain, SW))
        return jnp.where(self.bottom, fill, roll(a, -1, 0))

    def chain_up(self, a, fill):
        swapped = jnp.where(self.even, roll(fill, -DEEP, 1), roll(fill, DEEP, 1))
        return jnp.where(self.chain_top, swapped, roll(a, 1, 0))

    def chain_west(self, a, fill, beyond=None):
        swapped = jnp.where(self.even, roll(fill, DEEP, 1), roll(fill, -DEEP, 1))
        if beyond is not None:
            swapped = jnp.where(self.seventh, beyond, swapped)
        return jnp.where(self.chain_left, swapped, roll(a, 1, 1))

    def neighbours(self, minus0, plus0, minus1, plus1, beyond=None, main_only=False):
        n, s, ew, m, c = "n", "s", "ew", "m", "c"
        out = {
            m: (
                self.main_up(plus0[m], minus0[n]),
                self.main_down(minus0[m], minus0[s]),
                self.main_west(plus1[m], minus1[ew]),
                self.main_east(minus1[m], minus1[ew]),
            )
        }
        if main_only:
            return out
        top, bottom = minus0[m][:1], plus0[m][self.last :]
        for part, row, west, east in ((n, top, NW, NE), (s, bottom, SW, SE)):
            out[part] = (
                self.band_toward(plus0[part], row),
                roll(minus0[part], -1, 0),
                self.band_west(plus1[part], self.chain(minus1[c], west)),
                self.band_east(minus1[part], self.chain(minus1[c], east)),
            )
        out[ew] = (
            self.ew_up(plus0[ew], minus0[c]),
            self.ew_down(minus0[ew], minus0[c]),
            self.ew_toward(plus1[ew], plus1[m], minus1[m]),
            roll(minus1[ew], -1, 1),
        )
        out[c] = (
            self.chain_up(plus0[c], minus0[c]),
            roll(minus0[c], -1, 0),
            self.chain_west(plus1[c], minus1[c], beyond),
            roll(minus1[c], -1, 1),
        )
        return out


PARTS = ("m", "n", "s", "ew", "c")


def evolve(levels, gathered_count, panels, slots, *refs):
    pair, flip, diffusion, vertical, prior = refs[:5]
    refs = refs[5:]
    messages, refs = refs[:gathered_count], refs[gathered_count:]
    directions, refs = refs[:levels], refs[levels:]
    winds, refs = refs[:levels], refs[levels:]
    residuals, refs = refs[:levels], refs[levels:]
    image_out, sums_out = refs[:2]
    (
        table,
        x_main,
        w_main,
        images,
        x_band,
        w_band,
        x_ew,
        w_ew,
        x_chain,
        w_chain,
        x_far,
        g_main,
        g_band,
        g_ew,
        g_chain,
        obs,
        square,
    ) = refs[2:]
    width = directions[0].shape[0]
    last = width - 1
    tiles, subs = lax.axis_size("tile"), lax.axis_size("sub")
    tile, sub = lax.axis_index("tile"), lax.axis_index("sub")
    me = tile * subs + sub
    rows = table.shape[1]
    if gathered_count == 1:
        table[...] = messages[0][...]
    else:
        for index in range(gathered_count):
            xt, xs = index // subs, index % subs
            table[(tile ^ xt) * subs + (sub ^ xs)] = messages[index][...]
    for k in range(levels):
        level = rotated(levels, k)
        x_main[level] = directions[k][...]
        w_main[level] = winds[k][...]

    lane8 = iota((DEEP, LANES), 1)
    straight, reverse = lane8 % DEEP, last - lane8 % DEEP
    slot_of = lane8 // DEEP

    def band(panel, side, level, field):
        start = pl.multiple_of(level * BAND + (side * FIELDS + field) * DEEP, 8)
        return table[panel, pl.ds(start, DEEP), :]

    def lookup(panel, side):
        at = SIDES * panel + side
        other = pair[at]
        return lax.shift_right_logical(other, 2), other & 3, flip[at]

    def cross_row(sheet):
        panel, row_side, col_side = sheet
        panel, side, flipped = lookup(panel, row_side)
        end = (col_side & 1) ^ flipped
        return panel, side, end + jnp.where(side < 2, 2, 0)

    def cross_col(sheet):
        panel, row_side, col_side = sheet
        panel, side, flipped = lookup(panel, col_side)
        end = (row_side & 1) ^ flipped
        return panel, end + jnp.where(side < 2, 2, 0), side

    partners = [lookup(me, side) for side in range(SIDES)]
    for level in range(levels):
        turned = [[None] * FIELDS for _ in range(SIDES)]
        for side, (panel, other, flipped) in enumerate(partners):
            order = jnp.where(flipped == 1, last - lane8, lane8)
            sign = jnp.where(flipped == 1, -1.0, 1.0).astype(F32)
            for field in range(FIELDS):
                values = jnp.take_along_axis(band(panel, other, level, field), order, axis=1)
                turned[side][field] = values * sign if field == 2 else values
        for index in range(2):
            x_band[level, index] = turned[index][0]
            w_band[level, index, 0] = turned[index][1]
            w_band[level, index, 1] = turned[index][2]
        square[...] = jnp.zeros((width, LANES), F32)
        for field, target in ((0, None), (2, 0), (1, 1)):
            square[:DEEP, :] = turned[3][field]
            square[LANES // 2 : LANES // 2 + DEEP, :] = turned[2][field]
            if target is None:
                x_ew[level] = square[...].T
            else:
                w_ew[level, target] = square[...].T

    keys, kinds = [], []
    for corner, (row_side, col_side) in enumerate(CORNERS):
        start = (me, jnp.int32(row_side), jnp.int32(col_side))
        sheets = {0: start}
        ahead, behind = start, start
        for k in range(DEEP):
            ahead = cross_row(ahead) if k % 2 == 0 else cross_col(ahead)
            behind = cross_col(behind) if k % 2 == 0 else cross_row(behind)
            sheets[k + 1], sheets[-k - 1] = ahead, behind
        filled = [[jnp.zeros((DEEP, LANES), F32)] * FIELDS for _ in range(levels)]
        key = jnp.full((1, LANES), -1, jnp.int32)
        kind = jnp.full((1, LANES), -1, jnp.int32)
        for k, (panel, side, other) in sheets.items():
            end = other & 1
            order = jnp.where(end == 1, reverse, straight)
            sign = jnp.where(end == 1, -1.0, 1.0).astype(F32)
            if k == DEEP:
                for level in range(levels):
                    x_far[level, corner * DEEP : (corner + 1) * DEEP, :] = jnp.take_along_axis(
                        band(panel, side, level, 0), order, axis=1
                    )
                continue
            here = slot_of == k % SHEETS
            for level in range(levels):
                for field in range(FIELDS):
                    values = jnp.take_along_axis(band(panel, side, level, field), order, axis=1)
                    values = values * sign if field == 2 else values
                    filled[level][field] = jnp.where(here, values, filled[level][field])
            if abs(k) <= STEPS:
                key = jnp.where(here[:1], panel * width + order[:1], key)
                kind = jnp.where(here[:1], side, kind)
        keys.append(key)
        kinds.append(kind)
        place = slice(corner * DEEP, (corner + 1) * DEEP)
        for level in range(levels):
            x_chain[level, place, :] = filled[level][0]
            w_chain[level, 0, place, :] = filled[level][1]
            w_chain[level, 1, place, :] = filled[level][2]

    pairs = level_pairs(levels)
    depth_rows = record_rows(levels)
    base = levels * BAND
    fold = LANES // slots
    lane_rec = iota((depth_rows, LANES), 1)
    chunk_tiles = obs.shape[2] // LANES
    for group in range(panels // fold):
        packed = table[group * fold, base : base + depth_rows, :]
        for part in range(1, fold):
            shifted = roll(table[group * fold + part, base : base + depth_rows, :], part * slots, 1)
            packed = jnp.where(lane_rec // slots == part, shifted, packed)
        column = (group % chunk_tiles) * LANES
        obs[group // chunk_tiles, :, column : column + LANES] = packed
    chunks = obs.shape[0]
    span = obs.shape[2]
    key_columns = jnp.concatenate(keys, axis=0)
    kind_columns = jnp.concatenate(kinds, axis=0)
    key_tall = jnp.concatenate(
        [key_columns, kind_columns, jnp.zeros((LANES - 8, LANES), jnp.int32)], axis=0
    ).astype(F32).T
    comps = STEPS * len(pairs)

    def hits(mask):
        return jnp.where(mask, 1.0, 0.0).astype(BF16)

    def accumulate(chunk, _):
        data = obs[chunk]
        panel = data[0:1].astype(jnp.int32)
        oi = data[1:2].astype(jnp.int32)
        oj = data[2:3].astype(jnp.int32)
        when = data[3:4].astype(jnp.int32)
        tall = iota((width, span), 0)
        short = iota((DEEP, span), 0)
        at_row = jnp.where(tall == oi, 1.0, 0.0)
        at_row_here = jnp.where(panel == me, at_row, 0.0)
        at_col = jnp.where(tall == oj, 1.0, 0.0)
        at_row_b, at_col_b = at_row.astype(BF16), at_col.astype(BF16)
        distance = (oi, last - oi, oj, last - oj)
        band_hit, band_place = [], []
        for q, r, f in partners:
            depth = jnp.where(r == 0, distance[0], jnp.where(r == 1, distance[1], jnp.where(r == 2, distance[2], distance[3])))
            along = jnp.where(r < 2, oj, oi)
            along = jnp.where(f == 1, last - along, along)
            band_hit.append(jnp.where(panel == q, jnp.where(short == depth, 1.0, 0.0), 0.0))
            band_place.append(hits(tall == along))
        spot = (panel * width + oj, panel * width + oi)
        chain_hit = [jnp.where(short == distance[side], 1.0, 0.0) for side in range(SIDES)]
        chain_place = []
        for corner in range(4):
            key = key_tall[:, corner : corner + 1].astype(jnp.int32)
            kind = key_tall[:, 4 + corner : 5 + corner].astype(jnp.int32)
            chain_place.append(
                [hits((key == spot[side // 2]) & (kind == side)) for side in range(SIDES)]
            )
        gs = []
        for t in range(STEPS):
            for index in range(len(pairs)):
                g = jnp.where(when == t + 1, data[4 + index : 5 + index], 0.0)
                high = g.astype(BF16).astype(F32)
                gs.append((high, g - high))

        def product(left, right):
            return lax.dot_general(left, right, NT, preferred_element_type=F32)

        def tall_rows(hit):
            return jnp.concatenate([hit * part for g in gs for part in g], axis=0).astype(BF16)

        def put(ref, at, value):
            if chunks == 1:
                ref[at] = value
            else:
                ref[at] = ref[at] + value

        for comp in range(comps):
            high, low = gs[comp]
            value = product((at_row_here * high).astype(BF16), at_col_b)
            value = value + product((at_row_here * low).astype(BF16), at_col_b)
            put(g_main, comp, value)
        for side in range(SIDES):
            value = product(tall_rows(band_hit[side]), band_place[side])
            for comp in range(comps):
                at = 2 * comp * DEEP
                put(g_band, (side, comp), value[at : at + DEEP] + value[at + DEEP : at + 2 * DEEP])
        lefts = [tall_rows(chain_hit[side]) for side in range(SIDES)]
        for corner in range(4):
            value = product(lefts[0], chain_place[corner][0])
            for side in range(1, SIDES):
                value = value + product(lefts[side], chain_place[corner][side])
            for comp in range(comps):
                at = 2 * comp * DEEP
                put(
                    g_chain,
                    (comp, slice(corner * DEEP, (corner + 1) * DEEP)),
                    value[at : at + DEEP] + value[at + DEEP : at + 2 * DEEP],
                )
        return 0

    if chunks == 1:
        accumulate(0, 0)
    else:
        g_main[...] = jnp.zeros(g_main.shape, F32)
        g_band[...] = jnp.zeros(g_band.shape, F32)
        g_chain[...] = jnp.zeros(g_chain.shape, F32)
        lax.fori_loop(0, chunks, accumulate, 0)
    for comp in range(comps):
        square[...] = jnp.zeros((width, LANES), F32)
        square[:DEEP, :] = g_band[3, comp]
        square[LANES // 2 : LANES // 2 + DEEP, :] = g_band[2, comp]
        g_ew[comp] = square[...].T

    geometry = Geometry(width)
    mix = [diffusion[level] for level in range(levels)]
    blend = [vertical[level] for level in range(levels)]
    center = [1.0 - 4.0 * mix[level] - 2.0 * blend[level] for level in range(levels)]

    def wind(level, axis, part):
        if part == "m":
            return w_main[level, axis]
        if part == "n":
            return w_band[level, 0, axis]
        if part == "s":
            return w_band[level, 1, axis]
        return (w_ew if part == "ew" else w_chain)[level, axis]

    def forward(states, beyond):
        out = []
        for level in range(levels):
            x = states[level]
            near = geometry.neighbours(x, x, x, x, None if beyond is None else beyond[level])
            result = {}
            for part in PARTS:
                up, down, west, east = near[part]
                p, q = wind(level, 0, part), wind(level, 1, part)
                value = center[level] * x[part] + mix[level] * ((up + down) + (west + east))
                value = value + p * (up - down) + q * (west - east)
                others = [states[k][part] for k in (level - 1, level + 1) if 0 <= k < levels]
                if others:
                    value = value + blend[level] * sum(others[1:], others[0])
                result[part] = value
            out.append(result)
        return out

    def adjoint(states, main_only):
        out = []
        parts = ("m",) if main_only else PARTS
        for level in range(levels):
            w = states[level]
            minus0, plus0, minus1, plus1 = {}, {}, {}, {}
            for part in PARTS:
                scaled = mix[level] * w[part]
                p, q = wind(level, 0, part) * w[part], wind(level, 1, part) * w[part]
                minus0[part], plus0[part] = scaled + p, scaled - p
                minus1[part], plus1[part] = scaled + q, scaled - q
            near = geometry.neighbours(minus0, plus0, minus1, plus1, None, main_only)
            result = {}
            for part in parts:
                up, down, west, east = near[part]
                value = center[level] * w[part] + ((up + down) + (west + east))
                for k in (level - 1, level + 1):
                    if 0 <= k < levels:
                        value = value + blend[k] * states[k][part]
                result[part] = value
            out.append(result)
        return out

    def gain(t, index, part):
        comp = t * len(pairs) + index
        if part == "m":
            return g_main[comp]
        if part == "n":
            return g_band[0, comp]
        if part == "s":
            return g_band[1, comp]
        return (g_ew if part == "ew" else g_chain)[comp]

    def force(t, states):
        out = []
        for level in range(levels):
            result = {}
            for part in PARTS:
                value = None
                for other in range(levels):
                    index = pairs.index((min(level, other), max(level, other)))
                    term = gain(t, index, part) * states[other][part]
                    value = term if value is None else value + term
                result[part] = value
            out.append(result)
        return out

    states = [
        {"m": x_main[k], "n": x_band[k, 0], "s": x_band[k, 1], "ew": x_ew[k], "c": x_chain[k]} for k in range(levels)
    ]
    forcing = []
    for step in range(STEPS):
        states = forward(states, [x_far[k] for k in range(levels)] if step == 0 else None)
        forcing.append(force(step, states))
    current = forcing[STEPS - 1]
    for step in range(STEPS - 1, 0, -1):
        current = adjoint(current, False)
        current = [{part: current[k][part] + forcing[step - 1][k][part] for part in PARTS} for k in range(levels)]
    current = adjoint(current, True)

    zero = jnp.zeros((1, LANES), F32)
    totals = [zero] * 4
    for k in range(levels):
        images[k] = prior[k] * x_main[k] + current[k]["m"]
    for k in range(levels):
        level = rotated(levels, k)
        image = images[level]
        residual, direction = residuals[k][...], directions[k][...]
        if k == 0:
            image_out[...] = image
        for index, term in enumerate((residual * residual, direction * image, residual * image, image * image)):
            totals[index] = totals[index] + jnp.sum(term, axis=0, keepdims=True)
    sums_out[...] = jnp.concatenate(totals + [zero] * 4, axis=0)


def update(*refs):
    parts = refs[:-7]
    increment, residual, direction, image, increment_new, residual_new, direction_new = refs[-7:]
    total = parts[0][...]
    for part in parts[1:]:
        total = total + part[...]
    total = jnp.sum(total, axis=1, keepdims=True)
    norm_old, curvature, cross, square = (total[index : index + 1] for index in range(4))
    alpha = norm_old / curvature
    norm_new = norm_old - 2.0 * alpha * cross + alpha * alpha * square
    ratio = norm_new / norm_old
    d = direction[...]
    increment_new[...] = increment[...] + alpha * d
    r = residual[...] - alpha * image[...]
    residual_new[...] = r
    direction_new[...] = r + ratio * d


def exchanged(value, axis, mask):
    count = lax.axis_size(axis)
    return lax.ppermute(value, axis, [(i, i ^ mask) for i in range(count)])


def level_parts(value):
    count = lax.axis_size("lev")
    return [value] + [
        lax.ppermute(value, "lev", [(i, (i + k) % count) for i in range(count)]) for k in range(1, count)
    ]


def body(
    increment,
    residual,
    direction,
    wind_u,
    wind_v,
    diffusion,
    vertical,
    background_inv,
    side_pair,
    side_flip,
    obs_column,
    obs_time,
    obs_count,
    jacobian,
    error_inv,
):
    width = increment.shape[2]
    slots, _, channels = jacobian.shape
    tiles, subs, levels = lax.axis_size("tile"), lax.axis_size("sub"), lax.axis_size("lev")
    panels = tiles * subs
    shape = (width, width)
    flat = lambda a: a.reshape(shape)
    own = jacobian.reshape(slots, channels)
    bands, winds, wide = pl.pallas_call(
        prepare,
        out_shape=(
            jax.ShapeDtypeStruct((BAND, LANES), F32),
            jax.ShapeDtypeStruct((2,) + shape, F32),
            jax.ShapeDtypeStruct((slots, channels), F32),
        ),
        in_specs=[WHOLE] * 4,
        out_specs=(WHOLE,) * 3,
        name="prepare",
    )(flat(direction), flat(wind_u), flat(wind_v), own)
    all_bands = level_parts(bands)
    all_wide = level_parts(wide)
    all_winds = level_parts(winds)
    all_directions = level_parts(flat(direction))
    all_residuals = level_parts(flat(residual))

    area = width * width
    alive = jnp.arange(slots, dtype=jnp.int32) < obs_count[0]
    places = [jnp.where(alive, obs_column // area, -1), (obs_column % area) // width, obs_column % width, obs_time]
    place_rows = jnp.full((8, LANES), -1.0, F32)
    row_at = iota((8, LANES), 0)
    for index, values in enumerate(places):
        padded = jnp.pad(values, (0, LANES - slots), constant_values=-1).astype(F32)
        place_rows = jnp.where(row_at == index, padded[None, :], place_rows)

    rows = levels * BAND + record_rows(levels)
    message = pl.pallas_call(
        lambda *refs: compose(levels, *refs),
        out_shape=jax.ShapeDtypeStruct((rows, LANES), F32),
        in_specs=[WHOLE] * (2 * levels + 2),
        out_specs=WHOLE,
        scratch_shapes=[pltpu.VMEM((levels, slots, channels), F32)],
        name="compose",
    )(*all_bands, *all_wide, error_inv.reshape(1, channels), place_rows)

    if tiles <= 4:
        mine = [message] + [exchanged(message, "tile", mask) for mask in range(1, tiles)]
        messages = []
        for value in mine:
            messages += [value] + [exchanged(value, "sub", mask) for mask in range(1, subs)]
    else:
        messages = [lax.all_gather(message, ("tile", "sub"), axis=0)]

    span = min(CHUNK, panels * slots)
    pairs = len(level_pairs(levels))
    comps = STEPS * pairs
    chain = (SIDES * DEEP, LANES)
    vmem = lambda *dims: pltpu.VMEM(dims, F32)
    image, sums = pl.pallas_call(
        lambda *refs: evolve(levels, len(messages), panels, slots, *refs),
        out_shape=(jax.ShapeDtypeStruct(shape, F32), jax.ShapeDtypeStruct((8, LANES), F32)),
        in_specs=[SCALAR] * 5 + [WHOLE] * (len(messages) + 3 * levels),
        out_specs=(WHOLE, WHOLE),
        scratch_shapes=[
            vmem(panels, rows, LANES),
            vmem(levels, *shape),
            vmem(levels, 2, *shape),
            vmem(levels, *shape),
            vmem(levels, 2, DEEP, LANES),
            vmem(levels, 2, 2, DEEP, LANES),
            vmem(levels, width, LANES),
            vmem(levels, 2, width, LANES),
            vmem(levels, *chain),
            vmem(levels, 2, *chain),
            vmem(levels, *chain),
            vmem(comps, *shape),
            vmem(SIDES, comps, DEEP, LANES),
            vmem(comps, width, LANES),
            vmem(comps, *chain),
            vmem(panels * slots // span, record_rows(levels), span),
            vmem(width, LANES),
        ],
        name="evolve",
    )(
        side_pair.reshape(-1),
        side_flip.reshape(-1),
        diffusion,
        vertical,
        background_inv,
        *messages,
        *all_directions,
        *all_winds,
        *all_residuals,
    )

    for mask in range(1, subs):
        sums = sums + exchanged(sums, "sub", mask)
    if tiles <= 4:
        parts = [sums] + [exchanged(sums, "tile", mask) for mask in range(1, tiles)]
    else:
        mask = 1
        while mask < tiles:
            sums = sums + exchanged(sums, "tile", mask)
            mask *= 2
        parts = [sums]
    outputs = pl.pallas_call(
        update,
        out_shape=(jax.ShapeDtypeStruct(shape, F32),) * 3,
        in_specs=[WHOLE] * (len(parts) + 4),
        out_specs=(WHOLE,) * 3,
        name="update",
    )(*parts, flat(increment), flat(residual), flat(direction), image)
    return tuple(out.reshape(increment.shape) for out in outputs)


def solution(mesh):
    field = P(("member", "lev"), ("tile", "sub"), None)
    placed = (
        (field,) * 5
        + (P(),) * 5
        + (P(("tile", "sub")),) * 3
        + (P(("tile", "sub"), "lev", None), P())
    )
    return jax.shard_map(body, mesh=mesh, in_specs=placed, out_specs=(field,) * 3, check_vma=False)
```

```python
import functools

import jax
import jax.numpy as jnp
from jax import lax
from jax.experimental import pallas as pl
from jax.experimental.pallas import tpu as pltpu
from jax.sharding import PartitionSpec as P


STEPS = 4
DEEP = 2 * STEPS
SIDES = 4
FIELDS = 3
BAND = SIDES * FIELDS * DEEP
LANES = 128
CHAIN_AT = BAND
SHEETS = LANES // DEEP
CHUNK = 512
F32 = jnp.float32
BF16 = jnp.bfloat16
NT = (((1,), (1,)), ((), ()))
WHOLE = pl.BlockSpec(memory_space=pltpu.VMEM)
SCALAR = pl.BlockSpec(memory_space=pltpu.SMEM)
CORNERS = ((0, 2), (0, 3), (1, 2), (1, 3))
NW, NE, SW, SE = range(4)


def near(value):
    return pltpu.with_memory_space_constraint(value, pltpu.VMEM)


def limit(mebibytes):
    return pltpu.CompilerParams(vmem_limit_bytes=mebibytes << 20)


def iota(shape, axis):
    return lax.broadcasted_iota(jnp.int32, shape, axis)


def level_pairs(levels):
    return [(low, high) for low in range(levels) for high in range(low, levels)]


def record_rows(levels):
    return -(-(4 + len(level_pairs(levels))) // 8) * 8


def rotated(levels, k):
    return lax.rem(lax.axis_index("lev") + (levels - k), levels)


def prepare(bits, count, diffusion, vertical, prior, direction, wind_u, wind_v, residual, jacobian, columns, times, errors, bands, fields, wide, places, weights, scalars):
    x = direction[...]
    u = 0.5 * wind_u[...].astype(F32)
    v = 0.5 * wind_v[...].astype(F32)
    width = x.shape[0]
    wide[...] = jacobian[...].astype(F32)
    fields[0] = x
    fields[1] = u
    fields[2] = v
    fields[3] = residual[...]
    slots = columns.shape[1]
    column = columns[...]
    mask = (1 << bits) - 1
    alive = iota((1, slots), 1) < count[0]
    panel = jnp.where(alive, lax.shift_right_logical(column, 2 * bits), -1)
    rows = [panel, lax.shift_right_logical(column, bits) & mask, column & mask, times[...]]
    rows = jnp.concatenate(rows + rows, axis=0).astype(F32)
    if slots < LANES:
        rows = jnp.concatenate([rows, jnp.full((rows.shape[0], LANES - slots), -1.0, F32)], axis=1)
    places[...] = rows
    weights[...] = errors[...].reshape(1, -1)
    levels = diffusion.shape[0]
    scalars[...] = jnp.zeros(scalars.shape, F32)
    for index, values in enumerate((diffusion, vertical, prior)):
        for level in range(levels):
            at = index * levels + level
            scalars[at : at + 1, :] = jnp.full((1, LANES), values[level], F32)
    first = lambda a: a[:DEEP]
    last = lambda a: jnp.concatenate([a[width - 1 - d : width - d] for d in range(DEEP)], axis=0)
    xt, ut, vt = x.T, u.T, v.T
    parts = [
        (first(x), first(u), first(v)),
        (last(x), -last(u), last(v)),
        (first(xt), first(vt), first(ut)),
        (last(xt), -last(vt), last(ut)),
    ]
    for side in range(SIDES):
        for field in range(FIELDS):
            row = (side * FIELDS + field) * DEEP
            bands[row : row + DEEP, :] = parts[side][field]


def compose(levels, *refs):
    jacobians = refs[:levels]
    weights, places, record, ordered = refs[levels:]
    for k in range(levels):
        ordered[rotated(levels, k)] = jacobians[k][...]
    slots = ordered.shape[1]
    ones = jnp.ones((8, ordered.shape[2]), F32)
    scale = weights[...]
    rows = []
    for low, high in level_pairs(levels):
        product = ordered[low] * scale * ordered[high]
        total = lax.dot_general(ones, product, NT, precision=lax.Precision.HIGHEST, preferred_element_type=F32)
        rows.append(total[:1])
    spare = record_rows(levels) - 4 - len(rows)
    if spare:
        rows.append(jnp.zeros((spare, slots), F32))
    whole = jnp.concatenate(rows, axis=0)
    if slots < LANES:
        whole = jnp.concatenate([whole, jnp.zeros((whole.shape[0], LANES - slots), F32)], axis=1)
    record[...] = jnp.concatenate([places[:4, :], whole], axis=0)


def roll(a, shift, axis):
    return pltpu.roll(a, shift % a.shape[axis], axis)


class Geometry:
    def __init__(self, width):
        last = width - 1
        self.last = last
        row, lane = iota((width, LANES), 0), iota((width, LANES), 1)
        self.top, self.bottom = row == 0, row == last
        self.left, self.right = lane == 0, lane == last
        self.half = lane == LANES // 2
        brow, blane = iota((DEEP, LANES), 0), iota((DEEP, LANES), 1)
        self.band_first = brow == 0
        self.band_left, self.band_right = blane == 0, blane == last
        crow, clane = iota((SIDES * DEEP, LANES), 0), iota((SIDES * DEEP, LANES), 1)
        self.chain_top = crow % DEEP == 0
        self.chain_left = clane % DEEP == 0
        self.even = (clane // DEEP) % 2 == 0
        self.seventh = clane // DEEP == DEEP - 1
        self.near = iota((1, LANES), 1) < LANES // 2

    def chain(self, a, corner):
        return a[corner * DEEP : (corner + 1) * DEEP]

    def main_up(self, a, north):
        return jnp.where(self.top, north[:1], roll(a, 1, 0))

    def main_down(self, a, south):
        return jnp.where(self.bottom, south[:1], roll(a, -1, 0))

    def main_west(self, a, ew):
        return jnp.where(self.left, roll(ew, LANES // 2, 1), roll(a, 1, 1))

    def main_east(self, a, ew):
        return jnp.where(self.right, roll(ew, -1, 1), roll(a, -1, 1))

    def band_toward(self, a, main_row):
        return jnp.where(self.band_first, main_row, roll(a, 1, 0))

    def band_west(self, a, chain_block):
        return jnp.where(self.band_left, roll(chain_block, -2 * DEEP, 1), roll(a, 1, 1))

    def band_east(self, a, chain_block):
        return jnp.where(self.band_right, roll(chain_block, self.last - 2 * DEEP, 1), roll(a, -1, 1))

    def ew_toward(self, a, main_east, main_west):
        inner = jnp.where(self.half, roll(main_west, LANES // 2, 1), roll(a, 1, 1))
        return jnp.where(self.left, roll(main_east, 1, 1), inner)

    def ew_fill(self, east, west):
        return jnp.where(self.near, roll(east, 2 * DEEP, 1)[:1], roll(west, 2 * DEEP + LANES // 2, 1)[:1])

    def ew_up(self, a, chain):
        fill = self.ew_fill(self.chain(chain, NE), self.chain(chain, NW))
        return jnp.where(self.top, fill, roll(a, 1, 0))

    def ew_down(self, a, chain):
        fill = self.ew_fill(self.chain(chain, SE), self.chain(chain, SW))
        return jnp.where(self.bottom, fill, roll(a, -1, 0))

    def chain_up(self, a, fill):
        swapped = jnp.where(self.even, roll(fill, -DEEP, 1), roll(fill, DEEP, 1))
        return jnp.where(self.chain_top, swapped, roll(a, 1, 0))

    def chain_west(self, a, fill, beyond=None):
        swapped = jnp.where(self.even, roll(fill, DEEP, 1), roll(fill, -DEEP, 1))
        if beyond is not None:
            swapped = jnp.where(self.seventh, beyond, swapped)
        return jnp.where(self.chain_left, swapped, roll(a, 1, 1))

    def neighbours(self, minus0, plus0, minus1, plus1, beyond=None, main_only=False):
        n, s, ew, m, c = "n", "s", "ew", "m", "c"
        out = {
            m: (
                self.main_up(plus0[m], minus0[n]),
                self.main_down(minus0[m], minus0[s]),
                self.main_west(plus1[m], minus1[ew]),
                self.main_east(minus1[m], minus1[ew]),
            )
        }
        if main_only:
            return out
        top, bottom = minus0[m][:1], plus0[m][self.last :]
        for part, row, west, east in ((n, top, NW, NE), (s, bottom, SW, SE)):
            out[part] = (
                self.band_toward(plus0[part], row),
                roll(minus0[part], -1, 0),
                self.band_west(plus1[part], self.chain(minus1[c], west)),
                self.band_east(minus1[part], self.chain(minus1[c], east)),
            )
        out[ew] = (
            self.ew_up(plus0[ew], minus0[c]),
            self.ew_down(minus0[ew], minus0[c]),
            self.ew_toward(plus1[ew], plus1[m], minus1[m]),
            roll(minus1[ew], -1, 1),
        )
        out[c] = (
            self.chain_up(plus0[c], minus0[c]),
            roll(minus0[c], -1, 0),
            self.chain_west(plus1[c], minus1[c], beyond),
            roll(minus1[c], -1, 1),
        )
        return out


PARTS = ("m", "n", "s", "ew", "c")


def assemble(count, *refs):
    pair, flip = refs[:2]
    messages = refs[2 : 2 + count]
    parts, labels, table = refs[2 + count :]
    width = LANES
    last = width - 1
    subs = lax.axis_size("sub")
    tile, sub = lax.axis_index("tile"), lax.axis_index("sub")
    me = tile * subs + sub
    if count == 1:
        source = messages[0]
    else:
        source = table
        for index in range(count):
            xt, xs = index // subs, index % subs
            table[(tile ^ xt) * subs + (sub ^ xs)] = messages[index][...]

    lane8 = iota((DEEP, LANES), 1)
    straight, reverse = lane8 % DEEP, last - lane8 % DEEP
    slot_of = lane8 // DEEP

    def band(panel, side, field):
        start = pl.multiple_of((side * FIELDS + field) * DEEP, 8)
        return source[panel, pl.ds(start, DEEP), :]

    def lookup(panel, side):
        other = pair[side, panel]
        return lax.shift_right_logical(other, 2), other & 3, flip[side, panel]

    def cross_row(sheet):
        panel, row_side, col_side = sheet
        panel, side, flipped = lookup(panel, row_side)
        end = (col_side & 1) ^ flipped
        return panel, side, end + jnp.where(side < 2, 2, 0)

    def cross_col(sheet):
        panel, row_side, col_side = sheet
        panel, side, flipped = lookup(panel, col_side)
        end = (row_side & 1) ^ flipped
        return panel, end + jnp.where(side < 2, 2, 0), side

    for side in range(SIDES):
        panel, other, flipped = lookup(me, side)
        order = jnp.where(flipped == 1, last - lane8, lane8)
        sign = jnp.where(flipped == 1, -1.0, 1.0).astype(F32)
        for field in range(FIELDS):
            values = jnp.take_along_axis(band(panel, other, field), order, axis=1)
            at = (side * FIELDS + field) * DEEP
            parts[at : at + DEEP, :] = values * sign if field == 2 else values

    keys, kinds = [], []
    for corner, (row_side, col_side) in enumerate(CORNERS):
        start = (me, jnp.int32(row_side), jnp.int32(col_side))
        sheets = {0: start}
        ahead, behind = start, start
        for k in range(DEEP):
            ahead = cross_row(ahead) if k % 2 == 0 else cross_col(ahead)
            behind = cross_col(behind) if k % 2 == 0 else cross_row(behind)
            sheets[k + 1], sheets[-k - 1] = ahead, behind
        filled = [jnp.zeros((DEEP, LANES), F32)] * FIELDS
        key = jnp.full((1, LANES), -1, jnp.int32)
        kind = jnp.full((1, LANES), -1, jnp.int32)
        for k, (panel, side, other) in sheets.items():
            end = other & 1
            order = jnp.where(end == 1, reverse, straight)
            sign = jnp.where(end == 1, -1.0, 1.0).astype(F32)
            if k == DEEP:
                at = CHAIN_AT + (FIELDS * SIDES + corner) * DEEP
                parts[at : at + DEEP, :] = jnp.take_along_axis(band(panel, side, 0), order, axis=1)
                continue
            here = slot_of == k % SHEETS
            for field in range(FIELDS):
                values = jnp.take_along_axis(band(panel, side, field), order, axis=1)
                values = values * sign if field == 2 else values
                filled[field] = jnp.where(here, values, filled[field])
            if abs(k) <= STEPS:
                key = jnp.where(here[:1], panel * width + order[:1], key)
                kind = jnp.where(here[:1], side, kind)
        keys.append(key)
        kinds.append(kind)
        for field in range(FIELDS):
            at = CHAIN_AT + (field * SIDES + corner) * DEEP
            parts[at : at + DEEP, :] = filled[field]
    labels[...] = jnp.concatenate(keys + kinds, axis=0).astype(F32)


def gains(levels, slots, count, *refs):
    pair, flip, labels = refs[:3]
    records = refs[3 : 3 + count]
    g_main, g_band, g_ew, g_chain, obs, square = refs[3 + count :]
    width = LANES
    last = width - 1
    subs = lax.axis_size("sub")
    me = lax.axis_index("tile") * subs + lax.axis_index("sub")
    pairs = level_pairs(levels)
    depth_rows = record_rows(levels)
    fold = LANES // slots
    lane_rec = iota((depth_rows, LANES), 1)
    chunks, _, span = obs.shape
    chunk_tiles = span // LANES
    pieces = []
    for ref in records:
        if len(ref.shape) == 3:
            pieces += [ref[index] for index in range(ref.shape[0])]
        else:
            pieces += [ref[at : at + depth_rows, :] for at in range(0, ref.shape[0], depth_rows)]
    for group in range(len(pieces) // fold):
        packed = pieces[group * fold]
        for part in range(1, fold):
            shifted = roll(pieces[group * fold + part], part * slots, 1)
            packed = jnp.where(lane_rec // slots == part, shifted, packed)
        column = (group % chunk_tiles) * LANES
        obs[group // chunk_tiles, :, column : column + LANES] = packed
    label_tall = jnp.concatenate([labels[...], jnp.zeros((LANES - 8, LANES), F32)], axis=0).T
    comps = STEPS * len(pairs)
    partners = []
    for side in range(SIDES):
        other = pair[side, me]
        partners.append((lax.shift_right_logical(other, 2), other & 3, flip[side, me]))

    def hits(mask):
        return jnp.where(mask, 1.0, 0.0).astype(BF16)

    def accumulate(chunk, _):
        data = obs[chunk]
        panel = data[0:1].astype(jnp.int32)
        oi = data[1:2].astype(jnp.int32)
        oj = data[2:3].astype(jnp.int32)
        when = data[3:4].astype(jnp.int32)
        tall = iota((width, span), 0)
        short = iota((DEEP, span), 0)
        at_row = jnp.where(tall == oi, 1.0, 0.0)
        at_row_here = jnp.where(panel == me, at_row, 0.0)
        at_col = jnp.where(tall == oj, 1.0, 0.0)
        at_row_b, at_col_b = at_row.astype(BF16), at_col.astype(BF16)
        distance = (oi, last - oi, oj, last - oj)
        band_hit, band_place = [], []
        for q, r, f in partners:
            depth = jnp.where(r == 0, distance[0], jnp.where(r == 1, distance[1], jnp.where(r == 2, distance[2], distance[3])))
            along = jnp.where(r < 2, oj, oi)
            along = jnp.where(f == 1, last - along, along)
            band_hit.append(jnp.where(panel == q, jnp.where(short == depth, 1.0, 0.0), 0.0))
            band_place.append(hits(tall == along))
        spot = (panel * width + oj, panel * width + oi)
        chain_hit = [jnp.where(short == distance[side], 1.0, 0.0) for side in range(SIDES)]
        chain_place = []
        for corner in range(4):
            key = label_tall[:, corner : corner + 1].astype(jnp.int32)
            kind = label_tall[:, 4 + corner : 5 + corner].astype(jnp.int32)
            chain_place.append(
                [hits((key == spot[side // 2]) & (kind == side)) for side in range(SIDES)]
            )
        gs = []
        for t in range(STEPS):
            for index in range(len(pairs)):
                g = jnp.where(when == t + 1, data[4 + index : 5 + index], 0.0)
                high = g.astype(BF16).astype(F32)
                gs.append((high, g - high))

        def product(left, right):
            return lax.dot_general(left, right, NT, preferred_element_type=F32)

        def tall_rows(hit):
            return jnp.concatenate([hit * part for g in gs for part in g], axis=0).astype(BF16)

        def put(ref, at, value):
            if chunks == 1:
                ref[at] = value
            else:
                ref[at] = ref[at] + value

        for comp in range(comps):
            high, low = gs[comp]
            value = product((at_row_here * high).astype(BF16), at_col_b)
            value = value + product((at_row_here * low).astype(BF16), at_col_b)
            put(g_main, comp, value)
        for side in range(SIDES):
            value = product(tall_rows(band_hit[side]), band_place[side])
            for comp in range(comps):
                at = 2 * comp * DEEP
                total = value[at : at + DEEP] + value[at + DEEP : at + 2 * DEEP]
                if side < 2:
                    put(g_band, (side, comp), total)
                else:
                    put(square, (side - 2, comp), total)
        lefts = [tall_rows(chain_hit[side]) for side in range(SIDES)]
        for corner in range(4):
            value = product(lefts[0], chain_place[corner][0])
            for side in range(1, SIDES):
                value = value + product(lefts[side], chain_place[corner][side])
            for comp in range(comps):
                at = 2 * comp * DEEP
                put(
                    g_chain,
                    (comp, slice(corner * DEEP, (corner + 1) * DEEP)),
                    value[at : at + DEEP] + value[at + DEEP : at + 2 * DEEP],
                )
        return 0

    if chunks == 1:
        accumulate(0, 0)
    else:
        g_main[...] = jnp.zeros(g_main.shape, F32)
        g_band[...] = jnp.zeros(g_band.shape, F32)
        g_chain[...] = jnp.zeros(g_chain.shape, F32)
        square[...] = jnp.zeros(square.shape, F32)
        lax.fori_loop(0, chunks, accumulate, 0)
    for comp in range(comps):
        g_ew[comp] = side_by_side(square[1, comp], square[0, comp])


def side_by_side(east, west):
    gap = jnp.zeros((LANES // 2 - DEEP, LANES), F32)
    return jnp.concatenate([east, gap, west, gap], axis=0).T


def evolve(levels, *refs):
    scalars, refs = refs[0], refs[1:]
    diffusion, vertical, prior = (
        [scalars[index * levels + level : index * levels + level + 1, :] for level in range(levels)] for index in range(3)
    )
    parts, refs = refs[:levels], refs[levels:]
    fields, refs = refs[:levels], refs[levels:]
    g_main, g_band, g_ew, g_chain = refs[:4]
    image_out, sums_out, x_main, w_main, images, x_band, w_band, x_ew, w_ew, x_chain, w_chain, x_far = refs[4:]
    width = LANES
    pairs = level_pairs(levels)
    for k in range(levels):
        level = rotated(levels, k)
        x_main[level] = fields[k][0]
        w_main[level, 0] = fields[k][1]
        w_main[level, 1] = fields[k][2]
        part = parts[k]
        piece = lambda side, field: part[(side * FIELDS + field) * DEEP : (side * FIELDS + field + 1) * DEEP, :]
        for index in range(2):
            x_band[level, index] = piece(index, 0)
            w_band[level, index, 0] = piece(index, 1)
            w_band[level, index, 1] = piece(index, 2)
        x_ew[level] = side_by_side(piece(3, 0), piece(2, 0))
        w_ew[level, 0] = side_by_side(piece(3, 2), piece(2, 2))
        w_ew[level, 1] = side_by_side(piece(3, 1), piece(2, 1))
        chain = lambda field: part[CHAIN_AT + field * SIDES * DEEP : CHAIN_AT + (field + 1) * SIDES * DEEP, :]
        x_chain[level] = chain(0)
        w_chain[level, 0] = chain(1)
        w_chain[level, 1] = chain(2)
        x_far[level] = chain(3)

    geometry = Geometry(width)
    mix = [diffusion[level] for level in range(levels)]
    blend = [vertical[level] for level in range(levels)]
    center = [1.0 - 4.0 * mix[level] - 2.0 * blend[level] for level in range(levels)]

    def wind(level, axis, part):
        if part == "m":
            return w_main[level, axis]
        if part == "n":
            return w_band[level, 0, axis]
        if part == "s":
            return w_band[level, 1, axis]
        return (w_ew if part == "ew" else w_chain)[level, axis]

    def forward(states, beyond):
        out = []
        for level in range(levels):
            x = states[level]
            near = geometry.neighbours(x, x, x, x, None if beyond is None else beyond[level])
            result = {}
            for part in PARTS:
                up, down, west, east = near[part]
                p, q = wind(level, 0, part), wind(level, 1, part)
                value = center[level] * x[part] + mix[level] * ((up + down) + (west + east))
                value = value + p * (up - down) + q * (west - east)
                others = [states[k][part] for k in (level - 1, level + 1) if 0 <= k < levels]
                if others:
                    value = value + blend[level] * sum(others[1:], others[0])
                result[part] = value
            out.append(result)
        return out

    def adjoint(states, main_only):
        out = []
        parts = ("m",) if main_only else PARTS
        for level in range(levels):
            w = states[level]
            minus0, plus0, minus1, plus1 = {}, {}, {}, {}
            for part in PARTS:
                scaled = mix[level] * w[part]
                p, q = wind(level, 0, part) * w[part], wind(level, 1, part) * w[part]
                minus0[part], plus0[part] = scaled + p, scaled - p
                minus1[part], plus1[part] = scaled + q, scaled - q
            near = geometry.neighbours(minus0, plus0, minus1, plus1, None, main_only)
            result = {}
            for part in parts:
                up, down, west, east = near[part]
                value = center[level] * w[part] + ((up + down) + (west + east))
                for k in (level - 1, level + 1):
                    if 0 <= k < levels:
                        value = value + blend[k] * states[k][part]
                result[part] = value
            out.append(result)
        return out

    def gain(t, index, part):
        comp = t * len(pairs) + index
        if part == "m":
            return g_main[comp]
        if part == "n":
            return g_band[0, comp]
        if part == "s":
            return g_band[1, comp]
        return (g_ew if part == "ew" else g_chain)[comp]

    def force(t, states):
        out = []
        for level in range(levels):
            result = {}
            for part in PARTS:
                value = None
                for other in range(levels):
                    index = pairs.index((min(level, other), max(level, other)))
                    term = gain(t, index, part) * states[other][part]
                    value = term if value is None else value + term
                result[part] = value
            out.append(result)
        return out

    states = [
        {"m": x_main[k], "n": x_band[k, 0], "s": x_band[k, 1], "ew": x_ew[k], "c": x_chain[k]} for k in range(levels)
    ]
    forcing = []
    for step in range(STEPS):
        states = forward(states, [x_far[k] for k in range(levels)] if step == 0 else None)
        forcing.append(force(step, states))
    current = forcing[STEPS - 1]
    for step in range(STEPS - 1, 0, -1):
        current = adjoint(current, False)
        current = [{part: current[k][part] + forcing[step - 1][k][part] for part in PARTS} for k in range(levels)]
    current = adjoint(current, True)

    zero = jnp.zeros((1, LANES), F32)
    totals = [zero] * 4
    for k in range(levels):
        images[k] = prior[k] * x_main[k] + current[k]["m"]
    for k in range(levels):
        level = rotated(levels, k)
        image = images[level]
        residual, direction = fields[k][3], fields[k][0]
        if k == 0:
            image_out[...] = image
        for index, term in enumerate((residual * residual, direction * image, residual * image, image * image)):
            totals[index] = totals[index] + jnp.sum(term, axis=0, keepdims=True)
    sums_out[...] = jnp.concatenate(totals + [zero] * 4, axis=0)


def update(*refs):
    parts = refs[:-7]
    increment, residual, direction, image, increment_new, residual_new, direction_new = refs[-7:]
    total = parts[0][...]
    for part in parts[1:]:
        total = total + part[...]
    total = jnp.sum(total, axis=1, keepdims=True)
    norm_old, curvature, cross, square = (total[index : index + 1] for index in range(4))
    alpha = norm_old / curvature
    norm_new = norm_old - 2.0 * alpha * cross + alpha * alpha * square
    ratio = norm_new / norm_old
    d = direction[...]
    increment_new[...] = increment[...] + alpha * d
    r = residual[...] - alpha * image[...]
    residual_new[...] = r
    direction_new[...] = r + ratio * d


def exchanged(value, axis, mask):
    count = lax.axis_size(axis)
    return lax.ppermute(value, axis, [(i, i ^ mask) for i in range(count)])


def gathered(value, joined):
    tiles, subs = lax.axis_size("tile"), lax.axis_size("sub")
    if tiles > 4:
        return [lax.all_gather(value, ("tile", "sub"), axis=0)]
    if joined:
        out = [value] + [exchanged(value, "tile", mask) for mask in range(1, tiles)]
        whole = jnp.concatenate(out, axis=0)
        return [whole] + [exchanged(whole, "sub", mask) for mask in range(1, subs)]
    out = [value] + [exchanged(value, "sub", mask) for mask in range(1, subs)]
    for mask in range(1, tiles):
        other = exchanged(value, "tile", mask)
        out += [other] + [exchanged(other, "sub", by) for by in range(1, subs)]
    return out


def level_parts(value):
    count = lax.axis_size("lev")
    return [value] + [lax.ppermute(value, "lev", [(i, (i + k) % count) for i in range(count)]) for k in range(1, count)]


def body(
    increment,
    residual,
    direction,
    wind_u,
    wind_v,
    diffusion,
    vertical,
    background_inv,
    side_pair,
    side_flip,
    obs_column,
    obs_time,
    obs_count,
    jacobian,
    error_inv,
):
    width = increment.shape[2]
    slots, _, channels = jacobian.shape
    tiles, subs, levels = lax.axis_size("tile"), lax.axis_size("sub"), lax.axis_size("lev")
    panels = tiles * subs
    shape = (width, width)
    flat = lambda a: a.reshape(shape)
    own = jacobian.reshape(slots, channels)
    depth_rows = record_rows(levels)
    row = lambda a: a.reshape(1, -1)
    scalar_rows = -(-3 * levels // 8) * 8
    bands, fields, wide, places, weights, scalars = pl.pallas_call(
        functools.partial(prepare, width.bit_length() - 1),
        out_shape=(
            pltpu.VMEM((BAND, LANES), F32),
            pltpu.VMEM((4,) + shape, F32),
            pltpu.VMEM((slots, channels), F32),
            pltpu.VMEM((8, LANES), F32),
            pltpu.VMEM((1, channels), F32),
            pltpu.VMEM((scalar_rows, LANES), F32),
        ),
        in_specs=[SCALAR] * 4 + [WHOLE] * 8,
        out_specs=(WHOLE,) * 6,
        compiler_params=limit(60),
        name="prepare",
    )(
        obs_count,
        diffusion,
        vertical,
        background_inv,
        flat(direction),
        flat(wind_u),
        flat(wind_v),
        flat(residual),
        own,
        row(obs_column),
        row(obs_time),
        error_inv,
    )
    all_wide = level_parts(wide)
    all_fields = level_parts(fields)

    record = pl.pallas_call(
        functools.partial(compose, levels),
        out_shape=pltpu.VMEM((depth_rows, LANES), F32),
        in_specs=[WHOLE] * (levels + 2),
        out_specs=WHOLE,
        scratch_shapes=[pltpu.VMEM((levels, slots, channels), F32)],
        compiler_params=limit(8),
        name="compose",
    )(*[near(a) for a in (*all_wide, weights, places)])
    messages, records = gathered(bands, False), gathered(record, True)

    pair, flip = side_pair.T, side_flip.T
    vmem = lambda *dims: pltpu.VMEM(dims, F32)
    parts, labels = pl.pallas_call(
        functools.partial(assemble, len(messages)),
        out_shape=(vmem(CHAIN_AT + 4 * SIDES * DEEP, LANES), vmem(8, LANES)),
        in_specs=[SCALAR] * 2 + [WHOLE] * len(messages),
        out_specs=(WHOLE, WHOLE),
        scratch_shapes=[vmem(panels, BAND, LANES)],
        compiler_params=limit(8),
        name="assemble",
    )(pair, flip, *[near(a) for a in messages])
    all_parts = level_parts(parts)

    span = min(CHUNK, panels * slots)
    comps = STEPS * len(level_pairs(levels))
    chain = (SIDES * DEEP, LANES)
    products = pl.pallas_call(
        functools.partial(gains, levels, slots, len(records)),
        out_shape=(vmem(comps, *shape), vmem(2, comps, DEEP, LANES), vmem(comps, *shape), vmem(comps, *chain)),
        in_specs=[SCALAR] * 2 + [WHOLE] * (1 + len(records)),
        out_specs=(WHOLE,) * 4,
        scratch_shapes=[vmem(panels * slots // span, depth_rows, span), vmem(2, comps, DEEP, LANES)],
        compiler_params=limit(16),
        name="gains",
    )(pair, flip, *[near(a) for a in (labels, *records)])

    image, sums = pl.pallas_call(
        functools.partial(evolve, levels),
        out_shape=(vmem(*shape), vmem(8, LANES)),
        in_specs=[WHOLE] * (2 * levels + 5),
        out_specs=(WHOLE, WHOLE),
        scratch_shapes=[
            vmem(levels, *shape),
            vmem(levels, 2, *shape),
            vmem(levels, *shape),
            vmem(levels, 2, DEEP, LANES),
            vmem(levels, 2, 2, DEEP, LANES),
            vmem(levels, *shape),
            vmem(levels, 2, *shape),
            vmem(levels, *chain),
            vmem(levels, 2, *chain),
            vmem(levels, *chain),
        ],
        compiler_params=limit(12),
        name="evolve",
    )(*[near(a) for a in (scalars, *all_parts, *all_fields, *products)])

    for mask in range(1, subs):
        sums = sums + exchanged(sums, "sub", mask)
    if tiles <= 4:
        parts = [sums] + [exchanged(sums, "tile", mask) for mask in range(1, tiles)]
    else:
        mask = 1
        while mask < tiles:
            sums = sums + exchanged(sums, "tile", mask)
            mask *= 2
        parts = [sums]
    outputs = pl.pallas_call(
        update,
        out_shape=(jax.ShapeDtypeStruct(shape, F32),) * 3,
        in_specs=[WHOLE] * (len(parts) + 4),
        out_specs=(WHOLE,) * 3,
        compiler_params=limit(4),
        name="update",
    )(*[near(a) for a in (*parts, flat(increment), flat(residual), flat(direction), image)])
    return tuple(out.reshape(increment.shape) for out in outputs)


def solution(mesh):
    field = P(("member", "lev"), ("tile", "sub"), None)
    placed = (
        (field,) * 5
        + (P(),) * 5
        + (P(("tile", "sub")),) * 3
        + (P(("tile", "sub"), "lev", None), P())
    )
    return jax.shard_map(body, mesh=mesh, in_specs=placed, out_specs=(field,) * 3, check_vma=False)
```

```python
import functools

import jax
import jax.numpy as jnp
from jax import lax
from jax.experimental import pallas as pl
from jax.experimental.pallas import tpu as pltpu
from jax.sharding import PartitionSpec as P


STEPS = 4
DEEP = 2 * STEPS
SIDES = 4
FIELDS = 3
BAND = SIDES * FIELDS * DEEP
LANES = 128
CHAIN_AT = BAND
SHEETS = LANES // DEEP
CHUNK = 512
F32 = jnp.float32
BF16 = jnp.bfloat16
NT = (((1,), (1,)), ((), ()))
WHOLE = pl.BlockSpec(memory_space=pltpu.VMEM)
SCALAR = pl.BlockSpec(memory_space=pltpu.SMEM)
CORNERS = ((0, 2), (0, 3), (1, 2), (1, 3))
NW, NE, SW, SE = range(4)


def near(value):
    return pltpu.with_memory_space_constraint(value, pltpu.VMEM)


def limit(mebibytes):
    return pltpu.CompilerParams(vmem_limit_bytes=mebibytes << 20)


def iota(shape, axis):
    return lax.broadcasted_iota(jnp.int32, shape, axis)


def level_pairs(levels):
    return [(low, high) for low in range(levels) for high in range(low, levels)]


def record_rows(levels):
    return -(-(4 + len(level_pairs(levels))) // 8) * 8


def rotated(levels, k):
    return lax.rem(lax.axis_index("lev") + (levels - k), levels)


def prepare(bits, count, diffusion, vertical, prior, direction, wind_u, wind_v, residual, jacobian, columns, times, errors, bands, fields, wide, places, weights, scalars):
    x = direction[...]
    u = 0.5 * wind_u[...].astype(F32)
    v = 0.5 * wind_v[...].astype(F32)
    width = x.shape[0]
    wide[...] = jacobian[...].astype(F32)
    fields[0] = x
    fields[1] = u
    fields[2] = v
    fields[3] = residual[...]
    slots = columns.shape[1]
    column = columns[...]
    mask = (1 << bits) - 1
    alive = iota((1, slots), 1) < count[0]
    panel = jnp.where(alive, lax.shift_right_logical(column, 2 * bits), -1)
    rows = [panel, lax.shift_right_logical(column, bits) & mask, column & mask, times[...]]
    rows = jnp.concatenate(rows + rows, axis=0).astype(F32)
    if slots < LANES:
        rows = jnp.concatenate([rows, jnp.full((rows.shape[0], LANES - slots), -1.0, F32)], axis=1)
    places[...] = rows
    weights[...] = errors[...].reshape(1, -1)
    levels = diffusion.shape[0]
    scalars[...] = jnp.zeros(scalars.shape, F32)
    for index, values in enumerate((diffusion, vertical, prior)):
        for level in range(levels):
            at = index * levels + level
            scalars[at : at + 1, :] = jnp.full((1, LANES), values[level], F32)
    first = lambda a: a[:DEEP]
    last = lambda a: jnp.concatenate([a[width - 1 - d : width - d] for d in range(DEEP)], axis=0)
    xt, ut, vt = x.T, u.T, v.T
    parts = [
        (first(x), first(u), first(v)),
        (last(x), -last(u), last(v)),
        (first(xt), first(vt), first(ut)),
        (last(xt), -last(vt), last(ut)),
    ]
    for side in range(SIDES):
        for field in range(FIELDS):
            row = (side * FIELDS + field) * DEEP
            bands[row : row + DEEP, :] = parts[side][field]


def compose(levels, *refs):
    jacobians = refs[:levels]
    weights, places, record, ordered = refs[levels:]
    for k in range(levels):
        ordered[rotated(levels, k)] = jacobians[k][...]
    slots = ordered.shape[1]
    ones = jnp.ones((8, ordered.shape[2]), F32)
    scale = weights[...]
    rows = []
    for low, high in level_pairs(levels):
        product = ordered[low] * scale * ordered[high]
        total = lax.dot_general(ones, product, NT, precision=lax.Precision.HIGHEST, preferred_element_type=F32)
        rows.append(total[:1])
    spare = record_rows(levels) - 4 - len(rows)
    if spare:
        rows.append(jnp.zeros((spare, slots), F32))
    whole = jnp.concatenate(rows, axis=0)
    if slots < LANES:
        whole = jnp.concatenate([whole, jnp.zeros((whole.shape[0], LANES - slots), F32)], axis=1)
    record[...] = jnp.concatenate([places[:4, :], whole], axis=0)


def roll(a, shift, axis):
    return pltpu.roll(a, shift % a.shape[axis], axis)


class Geometry:
    def __init__(self, width):
        self.last = last = width - 1
        row, lane = iota((DEEP, LANES), 0), iota((DEEP, LANES), 1)
        self.band_first = row == 0
        self.left, self.right = lane == 0, lane == last
        self.near = lane < LANES // 2
        self.mirror = jnp.where(lane >= LANES - DEEP, 2 * LANES - 2 * DEEP + last - LANES - lane, lane)
        crow, clane = iota((SIDES * DEEP, LANES), 0), iota((SIDES * DEEP, LANES), 1)
        self.chain_top = crow % DEEP == 0
        self.chain_left = clane % DEEP == 0
        self.even = (clane // DEEP) % 2 == 0
        self.seventh = clane // DEEP == DEEP - 1

    def chain(self, a, corner):
        return a[corner * DEEP : (corner + 1) * DEEP]

    def band_west(self, a, chain_block):
        return jnp.where(self.left, roll(chain_block, -2 * DEEP, 1), roll(a, 1, 1))

    def band_east(self, a, chain_block):
        return jnp.where(self.right, roll(chain_block, self.last - 2 * DEEP, 1), roll(a, -1, 1))

    def column_fill(self, a, east, west):
        mirrored = jnp.take_along_axis(self.chain(a, west), self.mirror, axis=1)
        return jnp.where(self.near, roll(self.chain(a, east), 2 * DEEP, 1), mirrored)[:1]

    def chain_up(self, a, fill):
        swapped = jnp.where(self.even, roll(fill, -DEEP, 1), roll(fill, DEEP, 1))
        return jnp.where(self.chain_top, swapped, roll(a, 1, 0))

    def chain_west(self, a, fill, beyond=None):
        swapped = jnp.where(self.even, roll(fill, DEEP, 1), roll(fill, -DEEP, 1))
        if beyond is not None:
            swapped = jnp.where(self.seventh, beyond, swapped)
        return jnp.where(self.chain_left, swapped, roll(a, 1, 1))

    def across(self, main, columns):
        before_m, before_c = roll(main[0], 1, 1), roll(columns[0], 1, 1)
        after_m, after_c = roll(main[1], -1, 1), roll(columns[1], -1, 1)
        left, right = self.left, self.right
        return (
            (jnp.where(left, before_c, before_m), jnp.where(right, after_c, after_m)),
            (jnp.where(left, before_m, before_c), jnp.where(right, after_m, after_c)),
        )

    def neighbours(self, minus0, plus0, minus1, plus1, top, bottom, beyond=None):
        out = {}
        for part, row, west, east in (("n", top, NW, NE), ("s", bottom, SW, SE)):
            out[part] = (
                jnp.where(self.band_first, row, roll(plus0[part], 1, 0)),
                roll(minus0[part], -1, 0),
                self.band_west(plus1[part], self.chain(minus1["c"], west)),
                self.band_east(minus1[part], self.chain(minus1["c"], east)),
            )
        out["c"] = (
            self.chain_up(plus0["c"], minus0["c"]),
            roll(minus0["c"], -1, 0),
            self.chain_west(plus1["c"], minus1["c"], beyond),
            roll(minus1["c"], -1, 1),
        )
        return out


PARTS = ("n", "s", "c")
EDGE = 8


def assemble(count, *refs):
    pair, flip = refs[:2]
    messages = refs[2 : 2 + count]
    parts, labels, table = refs[2 + count :]
    width = LANES
    last = width - 1
    subs = lax.axis_size("sub")
    tile, sub = lax.axis_index("tile"), lax.axis_index("sub")
    me = tile * subs + sub
    if count == 1:
        source = messages[0]
    else:
        source = table
        for index in range(count):
            xt, xs = index // subs, index % subs
            table[(tile ^ xt) * subs + (sub ^ xs)] = messages[index][...]

    lane8 = iota((DEEP, LANES), 1)
    straight, reverse = lane8 % DEEP, last - lane8 % DEEP
    slot_of = lane8 // DEEP
    far_cell = (lane8 == DEEP * DEEP) & (iota((DEEP, LANES), 0) == 1)

    def band(panel, side, field):
        start = pl.multiple_of((side * FIELDS + field) * DEEP, 8)
        return source[panel, pl.ds(start, DEEP), :]

    def lookup(panel, side):
        other = pair[side, panel]
        return lax.shift_right_logical(other, 2), other & 3, flip[side, panel]

    def cross_row(sheet):
        panel, row_side, col_side = sheet
        panel, side, flipped = lookup(panel, row_side)
        end = (col_side & 1) ^ flipped
        return panel, side, end + jnp.where(side < 2, 2, 0)

    def cross_col(sheet):
        panel, row_side, col_side = sheet
        panel, side, flipped = lookup(panel, col_side)
        end = (row_side & 1) ^ flipped
        return panel, end + jnp.where(side < 2, 2, 0), side

    for side in range(SIDES):
        panel, other, flipped = lookup(me, side)
        order = jnp.where(flipped == 1, last - lane8, lane8)
        sign = jnp.where(flipped == 1, -1.0, 1.0).astype(F32)
        for field in range(FIELDS):
            values = jnp.take_along_axis(band(panel, other, field), order, axis=1)
            at = (side * FIELDS + field) * DEEP
            parts[at : at + DEEP, :] = values * sign if field == 2 else values

    keys = []
    panels = lax.axis_size("tile") * subs
    for corner, (row_side, col_side) in enumerate(CORNERS):
        start = (me, jnp.int32(row_side), jnp.int32(col_side))
        sheets = {0: start}
        ahead, behind = start, start
        for k in range(DEEP):
            ahead = cross_row(ahead) if k % 2 == 0 else cross_col(ahead)
            behind = cross_col(behind) if k % 2 == 0 else cross_row(behind)
            sheets[k + 1], sheets[-k - 1] = ahead, behind
        sheets[DEEP] = sheets.pop(DEEP)
        filled = [jnp.zeros((DEEP, LANES), F32)] * FIELDS
        key = jnp.full((1, LANES), -1, jnp.int32)
        for k, (panel, side, other) in sheets.items():
            end = other & 1
            order = jnp.where(end == 1, reverse, straight)
            sign = jnp.where(end == 1, -1.0, 1.0).astype(F32)
            if k == DEEP:
                values = roll(jnp.take_along_axis(band(panel, side, 0), order, axis=1), 1, 0)
                filled[0] = jnp.where(far_cell, values, filled[0])
                continue
            here = slot_of == k % SHEETS
            for field in range(FIELDS):
                values = jnp.take_along_axis(band(panel, side, field), order, axis=1)
                values = values * sign if field == 2 else values
                filled[field] = jnp.where(here, values, filled[field])
            if abs(k) <= STEPS:
                key = jnp.where(here[:1], (side * panels + panel) * width + order[:1], key)
        keys.append(key)
        for field in range(FIELDS):
            at = CHAIN_AT + (field * SIDES + corner) * DEEP
            parts[at : at + DEEP, :] = filled[field]
    lane = lane8[:1]
    sides = []
    for side in range(SIDES):
        panel, other, flipped = lookup(me, side)
        sides.append(jnp.where(lane == 0, panel, jnp.where(lane == 1, other, flipped)))
    labels[...] = jnp.concatenate(keys + sides, axis=0).astype(F32)


def gains(levels, slots, count, *refs):
    labels = refs[0]
    records = refs[1 : 1 + count]
    g_main, g_band, g_ew, g_chain, obs, square = refs[1 + count :]
    width = LANES
    last = width - 1
    subs = lax.axis_size("sub")
    me = lax.axis_index("tile") * subs + lax.axis_index("sub")
    panels = lax.axis_size("tile") * subs
    pairs = level_pairs(levels)
    depth_rows = record_rows(levels)
    fold = LANES // slots
    lane_rec = iota((depth_rows, LANES), 1)
    chunks, _, span = obs.shape
    chunk_tiles = span // LANES
    pieces = []
    for ref in records:
        if len(ref.shape) == 3:
            pieces += [ref[index] for index in range(ref.shape[0])]
        else:
            pieces += [ref[at : at + depth_rows, :] for at in range(0, ref.shape[0], depth_rows)]
    for group in range(len(pieces) // fold):
        packed = pieces[group * fold]
        for part in range(1, fold):
            shifted = roll(pieces[group * fold + part], part * slots, 1)
            packed = jnp.where(lane_rec // slots == part, shifted, packed)
        column = (group % chunk_tiles) * LANES
        obs[group // chunk_tiles, :, column : column + LANES] = packed
    label_tall = jnp.concatenate([labels[...], jnp.zeros((LANES - 8, LANES), F32)], axis=0).T
    comps = STEPS * len(pairs)
    partners = []
    for side in range(SIDES):
        row = labels[SIDES + side : SIDES + side + 1, :].astype(jnp.int32)
        partners.append((row[:, 0:1], row[:, 1:2], row[:, 2:3]))

    def hits(mask):
        return jnp.where(mask, 1.0, 0.0).astype(BF16)

    def accumulate(chunk, _):
        data = obs[chunk]
        panel = data[0:1].astype(jnp.int32)
        oi = data[1:2].astype(jnp.int32)
        oj = data[2:3].astype(jnp.int32)
        when = data[3:4].astype(jnp.int32)
        tall = iota((width, span), 0)
        at_row = jnp.where((tall == oi) & (panel == me), 1.0, 0.0)
        half = iota((DEEP, span), 0)
        first_half = half < STEPS
        shallow = half % STEPS
        distance = (oi, last - oi, oj, last - oj)
        pieces = []
        for index in range(len(pairs)):
            g = data[4 + index : 5 + index]
            high = g.astype(BF16).astype(F32)
            pieces.append((high, g - high))
        stacks = [jnp.where(first_half, high, low) for high, low in pieces]

        def product(left, right):
            return lax.dot_general(left, right, NT, preferred_element_type=F32)

        def put(ref, at, value):
            if chunks == 1:
                ref[at] = value
            else:
                ref[at] = ref[at] + value

        at_times = jnp.concatenate([hits((tall == oj) & (when == t + 1)) for t in range(STEPS)], axis=0)
        for index, (high, low) in enumerate(pieces):
            value = product((at_row * high).astype(BF16), at_times) + product((at_row * low).astype(BF16), at_times)
            for t in range(STEPS):
                put(g_main, t * len(pairs) + index, value[:, t * LANES : (t + 1) * LANES])

        def rows_of(depth):
            hit = jnp.where(shallow == depth, 1.0, 0.0)
            return jnp.concatenate(
                [jnp.where(when == t + 1, hit, 0.0) * stack for t in range(STEPS) for stack in stacks], axis=0
            ).astype(BF16)

        def joined(value, comp):
            part = value[comp * DEEP : (comp + 1) * DEEP]
            return part + roll(part, STEPS, 0)

        for side, (q, r, f) in enumerate(partners):
            depth = jnp.where(
                r == 0, distance[0], jnp.where(r == 1, distance[1], jnp.where(r == 2, distance[2], distance[3]))
            )
            along = jnp.where(r < 2, oj, oi)
            along = jnp.where(f == 1, last - along, along)
            value = product(rows_of(jnp.where(panel == q, depth, -1)), hits(tall == along))
            for comp in range(comps):
                if side < 2:
                    put(g_band, (side, comp), joined(value, comp))
                else:
                    put(square, (side - 2, comp), joined(value, comp))
        lefts = jnp.concatenate([rows_of(distance[side]) for side in range(SIDES)], axis=1)
        area = panels * width
        spots = [
            jnp.where(panel < 0, -2, panel * width + (oj if side < 2 else oi) + side * area) for side in range(SIDES)
        ]
        keys = [label_tall[:, corner : corner + 1].astype(jnp.int32) for corner in range(4)]
        for duo in range(2):
            places = jnp.concatenate(
                [
                    jnp.concatenate([hits(keys[corner] == spot) for spot in spots], axis=1)
                    for corner in (2 * duo, 2 * duo + 1)
                ],
                axis=0,
            )
            value = product(lefts, places)
            for comp in range(comps):
                total = joined(value, comp)
                for half_index in range(2):
                    corner = 2 * duo + half_index
                    put(
                        g_chain,
                        (comp, slice(corner * DEEP, (corner + 1) * DEEP)),
                        total[:, half_index * LANES : (half_index + 1) * LANES],
                    )
        return 0

    if chunks == 1:
        accumulate(0, 0)
    else:
        g_main[...] = jnp.zeros(g_main.shape, F32)
        g_band[...] = jnp.zeros(g_band.shape, F32)
        g_chain[...] = jnp.zeros(g_chain.shape, F32)
        square[...] = jnp.zeros(square.shape, F32)
        lax.fori_loop(0, chunks, accumulate, 0)
    for start in range(0, comps, DEEP):
        columns = as_columns([(square[1, comp], square[0, comp]) for comp in range(start, min(comps, start + DEEP))])
        for index, value in enumerate(columns):
            g_ew[start + index] = value


def as_columns(duos):
    groups = [jnp.zeros((DEEP, LANES), F32)] * SHEETS
    for index, (east, west) in enumerate(duos):
        groups[2 * index] = east
        groups[(2 * index - 1) % SHEETS] = jnp.concatenate([west[d : d + 1] for d in reversed(range(DEEP))], axis=0)
    columns = jnp.concatenate(groups, axis=0).T
    return [columns if index == 0 else roll(columns, -2 * DEEP * index, 1) for index in range(len(duos))]


def evolve(levels, *refs):
    scalars, refs = refs[0], refs[1:]
    mix, blend, prior = (
        [scalars[index * levels + level : index * levels + level + 1, :] for level in range(levels)] for index in range(3)
    )
    parts, refs = refs[:levels], refs[levels:]
    fields, refs = refs[:levels], refs[levels:]
    g_main, g_band, g_ew, g_chain = refs[:4]
    image_out, sums_out, x_main, x_ew, w_main, w_ew, f_main, f_ew, images, x_band, w_band, x_chain, w_chain, x_far = refs[4:]
    width = LANES
    pairs = level_pairs(levels)
    inner = slice(EDGE, EDGE + width)
    above, below = slice(EDGE - 1, EDGE), slice(EDGE + width, EDGE + width + 1)
    geometry = Geometry(width)
    for k in range(levels):
        level = rotated(levels, k)
        x_main[0, level, inner] = fields[k][0]
        w_main[level, 0, inner] = fields[k][1]
        w_main[level, 1, inner] = fields[k][2]
        part = parts[k]
        piece = lambda side, field: part[(side * FIELDS + field) * DEEP : (side * FIELDS + field + 1) * DEEP, :]
        for index in range(2):
            x_band[level, index] = piece(index, 0)
            w_band[level, index, 0] = piece(index, 1)
            w_band[level, index, 1] = piece(index, 2)
        columns = as_columns(
            [(piece(3, 0), piece(2, 0)), (piece(3, 2), piece(2, 2)), (piece(3, 1), -piece(2, 1))]
        )
        x_ew[0, level, inner], w_ew[level, 0, inner], w_ew[level, 1, inner] = columns
        chain = lambda field: part[CHAIN_AT + field * SIDES * DEEP : CHAIN_AT + (field + 1) * SIDES * DEEP, :]
        x_chain[level] = chain(0)
        w_chain[level, 0] = chain(1)
        w_chain[level, 1] = chain(2)
        x_far[level] = roll(roll(chain(0), -1, 0), -DEEP, 1)
        w_main[level, 0, above] = -piece(0, 1)[:1]
        w_main[level, 0, below] = piece(1, 1)[:1]
        w_ew[level, 0, above] = -geometry.column_fill(chain(1), NE, NW)
        w_ew[level, 0, below] = geometry.column_fill(chain(1), SE, SW)

    center = [1.0 - 4.0 * mix[level] - 2.0 * blend[level] for level in range(levels)]

    def wind(level, axis, part):
        if part == "c":
            return w_chain[level, axis]
        return w_band[level, 0 if part == "n" else 1, axis]

    def gain(t, low, high, part):
        comp = t * len(pairs) + pairs.index((min(low, high), max(low, high)))
        if part == "c":
            return g_chain[comp]
        return g_band[0 if part == "n" else 1, comp]

    def beside(level):
        return [k for k in (level - 1, level + 1) if 0 <= k < levels]

    def added(terms):
        total = terms[0]
        for term in terms[1:]:
            total = total + term
        return total

    def edges(now, states):
        for level in range(levels):
            state = states[level]
            x_main[now, level, above] = state["n"][:1]
            x_main[now, level, below] = state["s"][:1]
            x_ew[now, level, above] = geometry.column_fill(state["c"], NE, NW)
            x_ew[now, level, below] = geometry.column_fill(state["c"], SE, SW)

    def forward(t, states):
        now, then = t % 2, (t + 1) % 2
        edges(now, states)
        out = []
        for level in range(levels):
            x = states[level]
            top, bottom = x_main[now, level, EDGE : EDGE + 1], x_main[now, level, EDGE + width - 1 : EDGE + width]
            near = geometry.neighbours(x, x, x, x, top, bottom, x_far[level] if t == 0 else None)
            result = {}
            for part in PARTS:
                up, down, west, east = near[part]
                value = center[level] * x[part] + mix[level] * ((up + down) + (west + east))
                value = value + wind(level, 0, part) * (up - down) + wind(level, 1, part) * (west - east)
                for k in beside(level):
                    value = value + blend[level] * states[k][part]
                result[part] = value
            out.append(result)
        for start in range(EDGE, EDGE + width, 8):
            at, before, after = slice(start, start + 8), slice(start - 1, start + 7), slice(start + 1, start + 9)
            mains = [x_main[now, level, at] for level in range(levels)]
            columns = [x_ew[now, level, at] for level in range(levels)]
            fresh = ([], [])
            for level in range(levels):
                lanes = geometry.across((mains[level],) * 2, (columns[level],) * 2)
                for which, (x, w, own) in enumerate(((x_main, w_main, mains), (x_ew, w_ew, columns))):
                    up, down = x[now, level, before], x[now, level, after]
                    west, east = lanes[which]
                    value = center[level] * own[level] + mix[level] * ((up + down) + (west + east))
                    value = value + w[level, 0, at] * (up - down) + w[level, 1, at] * (west - east)
                    if beside(level):
                        value = value + blend[level] * added([own[k] for k in beside(level)])
                    fresh[which].append(value)
            rows = slice(start - EDGE, start - EDGE + 8)
            for which, (x, g, f) in enumerate(((x_main, g_main, f_main), (x_ew, g_ew, f_ew))):
                for level in range(levels):
                    if t < STEPS - 1:
                        x[then, level, at] = fresh[which][level]
                    terms = []
                    for other in range(levels):
                        comp = t * len(pairs) + pairs.index((min(level, other), max(level, other)))
                        terms.append(g[comp, rows] * fresh[which][other])
                    if t < STEPS - 1:
                        f[t, level, rows] = added(terms)
                    else:
                        x[then, level, at] = added(terms)
        forces = [
            {
                part: added([gain(t, level, other, part) * out[other][part] for other in range(levels)])
                for part in PARTS
            }
            for level in range(levels)
        ]
        return out, forces

    def adjoint(t, states, forces):
        now, then = (t + 1) % 2, t % 2
        edges(now, states)
        out = []
        for level in range(levels if forces is not None else 0):
            w = states[level]
            minus0, plus0, minus1, plus1 = {}, {}, {}, {}
            for part in PARTS:
                scaled = mix[level] * w[part]
                p, q = wind(level, 0, part) * w[part], wind(level, 1, part) * w[part]
                minus0[part], plus0[part] = scaled + p, scaled - p
                minus1[part], plus1[part] = scaled + q, scaled - q
            first, final = slice(EDGE, EDGE + 1), slice(EDGE + width - 1, EDGE + width)
            top = (mix[level] + w_main[level, 0, first]) * x_main[now, level, first]
            bottom = (mix[level] - w_main[level, 0, final]) * x_main[now, level, final]
            near = geometry.neighbours(minus0, plus0, minus1, plus1, top, bottom)
            result = {}
            for part in PARTS:
                up, down, west, east = near[part]
                value = center[level] * w[part] + ((up + down) + (west + east)) + forces[level][part]
                for k in beside(level):
                    value = value + blend[k] * states[k][part]
                result[part] = value
            out.append(result)
        for start in range(EDGE, EDGE + width, 8):
            at, before, after = slice(start, start + 8), slice(start - 1, start + 7), slice(start + 1, start + 9)
            rows = slice(start - EDGE, start - EDGE + 8)
            mains = [x_main[now, level, at] for level in range(levels)]
            columns = [x_ew[now, level, at] for level in range(levels)]
            for level in range(levels):
                given = []
                for w, own in ((w_main, mains), (w_ew, columns)):
                    scaled, turned = mix[level] * own[level], w[level, 1, at] * own[level]
                    given.append((scaled - turned, scaled + turned))
                lanes = geometry.across(*given)
                for which, (x, w, own, f) in enumerate(
                    ((x_main, w_main, mains, f_main), (x_ew, w_ew, columns, f_ew))
                ):
                    if which and forces is None:
                        continue
                    up = (mix[level] - w[level, 0, before]) * x[now, level, before]
                    down = (mix[level] + w[level, 0, after]) * x[now, level, after]
                    west, east = lanes[which]
                    value = center[level] * own[level] + ((up + down) + (west + east))
                    for k in beside(level):
                        value = value + blend[k] * own[k]
                    if forces is None:
                        images[level, rows] = value + prior[level] * x_start[level][rows]
                    else:
                        x[then, level, at] = value + f[t - 1, level, rows]
        return out

    x_start = [f_main.at[STEPS - 1, level] for level in range(levels)]
    for level in range(levels):
        x_start[level][...] = x_main[0, level, inner]
    states = [{"n": x_band[k, 0], "s": x_band[k, 1], "c": x_chain[k]} for k in range(levels)]
    forcing = []
    for t in range(STEPS):
        states, forces = forward(t, states)
        forcing.append(forces)
    current = forcing[STEPS - 1]
    for t in range(STEPS - 1, -1, -1):
        current = adjoint(t, current, forcing[t - 1] if t else None)

    zero = jnp.zeros((1, LANES), F32)
    totals = [zero] * 4
    for k in range(levels):
        image = images[rotated(levels, k)]
        residual, direction = fields[k][3], fields[k][0]
        if k == 0:
            image_out[...] = image
        for index, term in enumerate((residual * residual, direction * image, residual * image, image * image)):
            totals[index] = totals[index] + jnp.sum(term, axis=0, keepdims=True)
    sums_out[...] = jnp.concatenate(totals + [zero] * 4, axis=0)


def update(*refs):
    parts = refs[:-7]
    increment, residual, direction, image, increment_new, residual_new, direction_new = refs[-7:]
    total = parts[0][...]
    for part in parts[1:]:
        total = total + part[...]
    total = jnp.sum(total, axis=1, keepdims=True)
    norm_old, curvature, cross, square = (total[index : index + 1] for index in range(4))
    alpha = norm_old / curvature
    norm_new = norm_old - 2.0 * alpha * cross + alpha * alpha * square
    ratio = norm_new / norm_old
    d = direction[...]
    increment_new[...] = increment[...] + alpha * d
    r = residual[...] - alpha * image[...]
    residual_new[...] = r
    direction_new[...] = r + ratio * d


def exchanged(value, axis, mask):
    count = lax.axis_size(axis)
    return lax.ppermute(value, axis, [(i, i ^ mask) for i in range(count)])


def gathered(value, joined):
    tiles, subs = lax.axis_size("tile"), lax.axis_size("sub")
    if tiles > 4:
        return [lax.all_gather(value, ("tile", "sub"), axis=0)]
    if joined:
        out = [value] + [exchanged(value, "tile", mask) for mask in range(1, tiles)]
        whole = jnp.concatenate(out, axis=0)
        return [whole] + [exchanged(whole, "sub", mask) for mask in range(1, subs)]
    out = [value] + [exchanged(value, "sub", mask) for mask in range(1, subs)]
    for mask in range(1, tiles):
        other = exchanged(value, "tile", mask)
        out += [other] + [exchanged(other, "sub", by) for by in range(1, subs)]
    return out


def level_parts(value):
    count = lax.axis_size("lev")
    return [value] + [lax.ppermute(value, "lev", [(i, (i + k) % count) for i in range(count)]) for k in range(1, count)]


def body(
    increment,
    residual,
    direction,
    wind_u,
    wind_v,
    diffusion,
    vertical,
    background_inv,
    side_pair,
    side_flip,
    obs_column,
    obs_time,
    obs_count,
    jacobian,
    error_inv,
):
    width = increment.shape[2]
    slots, _, channels = jacobian.shape
    tiles, subs, levels = lax.axis_size("tile"), lax.axis_size("sub"), lax.axis_size("lev")
    panels = tiles * subs
    shape = (width, width)
    flat = lambda a: a.reshape(shape)
    own = jacobian.reshape(slots, channels)
    depth_rows = record_rows(levels)
    row = lambda a: a.reshape(1, -1)
    scalar_rows = -(-3 * levels // 8) * 8
    bands, fields, wide, places, weights, scalars = pl.pallas_call(
        functools.partial(prepare, width.bit_length() - 1),
        out_shape=(
            pltpu.VMEM((BAND, LANES), F32),
            pltpu.VMEM((4,) + shape, F32),
            pltpu.VMEM((slots, channels), F32),
            pltpu.VMEM((8, LANES), F32),
            pltpu.VMEM((1, channels), F32),
            pltpu.VMEM((scalar_rows, LANES), F32),
        ),
        in_specs=[SCALAR] * 4 + [WHOLE] * 8,
        out_specs=(WHOLE,) * 6,
        compiler_params=limit(60),
        name="prepare",
    )(
        obs_count,
        diffusion,
        vertical,
        background_inv,
        flat(direction),
        flat(wind_u),
        flat(wind_v),
        flat(residual),
        own,
        row(obs_column),
        row(obs_time),
        error_inv,
    )
    all_wide = level_parts(wide)
    all_fields = level_parts(fields)

    record = pl.pallas_call(
        functools.partial(compose, levels),
        out_shape=pltpu.VMEM((depth_rows, LANES), F32),
        in_specs=[WHOLE] * (levels + 2),
        out_specs=WHOLE,
        scratch_shapes=[pltpu.VMEM((levels, slots, channels), F32)],
        compiler_params=limit(8),
        name="compose",
    )(*[near(a) for a in (*all_wide, weights, places)])
    messages, records = gathered(bands, False), gathered(record, True)

    pair, flip = side_pair.T, side_flip.T
    vmem = lambda *dims: pltpu.VMEM(dims, F32)
    parts, labels = pl.pallas_call(
        functools.partial(assemble, len(messages)),
        out_shape=(vmem(CHAIN_AT + FIELDS * SIDES * DEEP, LANES), vmem(8, LANES)),
        in_specs=[SCALAR] * 2 + [WHOLE] * len(messages),
        out_specs=(WHOLE, WHOLE),
        scratch_shapes=[vmem(panels, BAND, LANES)],
        compiler_params=limit(8),
        name="assemble",
    )(pair, flip, *[near(a) for a in messages])
    all_parts = level_parts(parts)

    span = min(CHUNK, panels * slots)
    comps = STEPS * len(level_pairs(levels))
    chain = (SIDES * DEEP, LANES)
    padded = (width + 2 * EDGE, LANES)
    products = pl.pallas_call(
        functools.partial(gains, levels, slots, len(records)),
        out_shape=(vmem(comps, *shape), vmem(2, comps, DEEP, LANES), vmem(comps, *shape), vmem(comps, *chain)),
        in_specs=[WHOLE] * (1 + len(records)),
        out_specs=(WHOLE,) * 4,
        scratch_shapes=[vmem(panels * slots // span, depth_rows, span), vmem(2, comps, DEEP, LANES)],
        compiler_params=limit(16),
        name="gains",
    )(*[near(a) for a in (labels, *records)])

    image, sums = pl.pallas_call(
        functools.partial(evolve, levels),
        out_shape=(vmem(*shape), vmem(8, LANES)),
        in_specs=[WHOLE] * (2 * levels + 5),
        out_specs=(WHOLE, WHOLE),
        scratch_shapes=[
            vmem(2, levels, *padded),
            vmem(2, levels, *padded),
            vmem(levels, 2, *padded),
            vmem(levels, 2, *padded),
            vmem(STEPS, levels, *shape),
            vmem(STEPS, levels, *shape),
            vmem(levels, *shape),
            vmem(levels, 2, DEEP, LANES),
            vmem(levels, 2, 2, DEEP, LANES),
            vmem(levels, *chain),
            vmem(levels, 2, *chain),
            vmem(levels, *chain),
        ],
        compiler_params=limit(12),
        name="evolve",
    )(*[near(a) for a in (scalars, *all_parts, *all_fields, *products)])

    for mask in range(1, subs):
        sums = sums + exchanged(sums, "sub", mask)
    if tiles <= 4:
        parts = [sums] + [exchanged(sums, "tile", mask) for mask in range(1, tiles)]
    else:
        mask = 1
        while mask < tiles:
            sums = sums + exchanged(sums, "tile", mask)
            mask *= 2
        parts = [sums]
    outputs = pl.pallas_call(
        update,
        out_shape=(jax.ShapeDtypeStruct(shape, F32),) * 3,
        in_specs=[WHOLE] * (len(parts) + 4),
        out_specs=(WHOLE,) * 3,
        compiler_params=limit(4),
        name="update",
    )(*[near(a) for a in (*parts, flat(increment), flat(residual), flat(direction), image)])
    return tuple(out.reshape(increment.shape) for out in outputs)


def solution(mesh):
    field = P(("member", "lev"), ("tile", "sub"), None)
    placed = (
        (field,) * 5
        + (P(),) * 5
        + (P(("tile", "sub")),) * 3
        + (P(("tile", "sub"), "lev", None), P())
    )
    return jax.shard_map(body, mesh=mesh, in_specs=placed, out_specs=(field,) * 3, check_vma=False)
```

```python
import functools

import jax
import jax.numpy as jnp
from jax import lax
from jax.experimental import pallas as pl
from jax.experimental.pallas import tpu as pltpu
from jax.sharding import PartitionSpec as P


STEPS = 4
DEEP = 2 * STEPS
SIDES = 4
FIELDS = 3
BAND = SIDES * FIELDS * DEEP
LANES = 128
CHAIN_AT = BAND
SHEETS = LANES // DEEP
CHUNK = 512
F32 = jnp.float32
BF16 = jnp.bfloat16
NT = (((1,), (1,)), ((), ()))
WHOLE = pl.BlockSpec(memory_space=pltpu.VMEM)
SCALAR = pl.BlockSpec(memory_space=pltpu.SMEM)
CORNERS = ((0, 2), (0, 3), (1, 2), (1, 3))
NW, NE, SW, SE = range(4)


def near(value):
    return pltpu.with_memory_space_constraint(value, pltpu.VMEM)


def limit(mebibytes):
    return pltpu.CompilerParams(vmem_limit_bytes=mebibytes << 20)


def iota(shape, axis):
    return lax.broadcasted_iota(jnp.int32, shape, axis)


def level_pairs(levels):
    return [(low, high) for low in range(levels) for high in range(low, levels)]


def record_rows(levels):
    return -(-(4 + len(level_pairs(levels))) // 8) * 8


def rotated(levels, k):
    return lax.rem(lax.axis_index("lev") + (levels - k), levels)


def prepare(bits, count, diffusion, vertical, prior, direction, wind_u, wind_v, residual, jacobian, columns, times, errors, bands, fields, wide, places, weights, scalars):
    x = direction[...]
    u = 0.5 * wind_u[...].astype(F32)
    v = 0.5 * wind_v[...].astype(F32)
    width = x.shape[0]
    wide[...] = jacobian[...].astype(F32)
    fields[0] = x
    fields[1] = u
    fields[2] = v
    fields[3] = residual[...]
    slots = columns.shape[1]
    column = columns[...]
    mask = (1 << bits) - 1
    alive = iota((1, slots), 1) < count[0]
    panel = jnp.where(alive, lax.shift_right_logical(column, 2 * bits), -1)
    rows = [panel, lax.shift_right_logical(column, bits) & mask, column & mask, times[...]]
    rows = jnp.concatenate(rows + rows, axis=0).astype(F32)
    if slots < LANES:
        rows = jnp.concatenate([rows, jnp.full((rows.shape[0], LANES - slots), -1.0, F32)], axis=1)
    places[...] = rows
    weights[...] = errors[...].reshape(1, -1)
    levels = diffusion.shape[0]
    scalars[...] = jnp.zeros(scalars.shape, F32)
    for index, values in enumerate((diffusion, vertical, prior)):
        for level in range(levels):
            at = index * levels + level
            scalars[at : at + 1, :] = jnp.full((1, LANES), values[level], F32)
    first = lambda a: a[:DEEP]
    last = lambda a: jnp.concatenate([a[width - 1 - d : width - d] for d in range(DEEP)], axis=0)
    xt, ut, vt = x.T, u.T, v.T
    parts = [
        (first(x), first(u), first(v)),
        (last(x), -last(u), last(v)),
        (first(xt), first(vt), first(ut)),
        (last(xt), -last(vt), last(ut)),
    ]
    for side in range(SIDES):
        for field in range(FIELDS):
            row = (side * FIELDS + field) * DEEP
            bands[row : row + DEEP, :] = parts[side][field]


def compose(levels, *refs):
    jacobians = refs[:levels]
    weights, places, record, ordered = refs[levels:]
    for k in range(levels):
        ordered[rotated(levels, k)] = jacobians[k][...]
    slots = ordered.shape[1]
    ones = jnp.ones((8, ordered.shape[2]), F32)
    scale = weights[...]
    rows = []
    for low, high in level_pairs(levels):
        product = ordered[low] * scale * ordered[high]
        total = lax.dot_general(ones, product, NT, precision=lax.Precision.HIGHEST, preferred_element_type=F32)
        rows.append(total[:1])
    spare = record_rows(levels) - 4 - len(rows)
    if spare:
        rows.append(jnp.zeros((spare, slots), F32))
    whole = jnp.concatenate(rows, axis=0)
    if slots < LANES:
        whole = jnp.concatenate([whole, jnp.zeros((whole.shape[0], LANES - slots), F32)], axis=1)
    record[...] = jnp.concatenate([places[:4, :], whole], axis=0)


def roll(a, shift, axis):
    return pltpu.roll(a, shift % a.shape[axis], axis)


class Geometry:
    def __init__(self, width):
        self.last = last = width - 1
        row, lane = iota((DEEP, LANES), 0), iota((DEEP, LANES), 1)
        self.band_first = row == 0
        self.left, self.right = lane == 0, lane == last
        self.near = lane < LANES // 2
        self.mirror = jnp.where(lane >= LANES - DEEP, 2 * LANES - 2 * DEEP + last - LANES - lane, lane)
        crow, clane = iota((SIDES * DEEP, LANES), 0), iota((SIDES * DEEP, LANES), 1)
        self.chain_top = crow % DEEP == 0
        self.chain_left = clane % DEEP == 0
        self.even = (clane // DEEP) % 2 == 0
        self.seventh = clane // DEEP == DEEP - 1

    def chain(self, a, corner):
        return a[corner * DEEP : (corner + 1) * DEEP]

    def band_west(self, a, chain_block):
        return jnp.where(self.left, roll(chain_block, -2 * DEEP, 1), roll(a, 1, 1))

    def band_east(self, a, chain_block):
        return jnp.where(self.right, roll(chain_block, self.last - 2 * DEEP, 1), roll(a, -1, 1))

    def column_fill(self, a, east, west):
        mirrored = jnp.take_along_axis(self.chain(a, west), self.mirror, axis=1)
        return jnp.where(self.near, roll(self.chain(a, east), 2 * DEEP, 1), mirrored)[:1]

    def chain_up(self, a, fill):
        swapped = jnp.where(self.even, roll(fill, -DEEP, 1), roll(fill, DEEP, 1))
        return jnp.where(self.chain_top, swapped, roll(a, 1, 0))

    def chain_west(self, a, fill, beyond=None):
        swapped = jnp.where(self.even, roll(fill, DEEP, 1), roll(fill, -DEEP, 1))
        if beyond is not None:
            swapped = jnp.where(self.seventh, beyond, swapped)
        return jnp.where(self.chain_left, swapped, roll(a, 1, 1))

    def across(self, main, columns):
        before_m, before_c = roll(main[0], 1, 1), roll(columns[0], 1, 1)
        after_m, after_c = roll(main[1], -1, 1), roll(columns[1], -1, 1)
        left, right = self.left, self.right
        return (
            (jnp.where(left, before_c, before_m), jnp.where(right, after_c, after_m)),
            (jnp.where(left, before_m, before_c), jnp.where(right, after_m, after_c)),
        )

    def neighbours(self, minus0, plus0, minus1, plus1, top, bottom, beyond=None):
        out = {}
        for part, row, west, east in (("n", top, NW, NE), ("s", bottom, SW, SE)):
            out[part] = (
                jnp.where(self.band_first, row, roll(plus0[part], 1, 0)),
                roll(minus0[part], -1, 0),
                self.band_west(plus1[part], self.chain(minus1["c"], west)),
                self.band_east(minus1[part], self.chain(minus1["c"], east)),
            )
        out["c"] = (
            self.chain_up(plus0["c"], minus0["c"]),
            roll(minus0["c"], -1, 0),
            self.chain_west(plus1["c"], minus1["c"], beyond),
            roll(minus1["c"], -1, 1),
        )
        return out


PARTS = ("n", "s", "c")
EDGE = 8


def assemble(count, *refs):
    pair, flip = refs[:2]
    messages = refs[2 : 2 + count]
    parts, labels, table = refs[2 + count :]
    width = LANES
    last = width - 1
    subs = lax.axis_size("sub")
    tile, sub = lax.axis_index("tile"), lax.axis_index("sub")
    me = tile * subs + sub
    if count == 1:
        source = messages[0]
    else:
        source = table
        for index in range(count):
            xt, xs = index // subs, index % subs
            table[(tile ^ xt) * subs + (sub ^ xs)] = messages[index][...]

    lane8 = iota((DEEP, LANES), 1)
    straight, reverse = lane8 % DEEP, last - lane8 % DEEP
    slot_of = lane8 // DEEP
    far_cell = (lane8 == DEEP * DEEP) & (iota((DEEP, LANES), 0) == 1)

    def band(panel, side, field):
        start = pl.multiple_of((side * FIELDS + field) * DEEP, 8)
        return source[panel, pl.ds(start, DEEP), :]

    def lookup(panel, side):
        other = pair[side, panel]
        return lax.shift_right_logical(other, 2), other & 3, flip[side, panel]

    def cross_row(sheet):
        panel, row_side, col_side = sheet
        panel, side, flipped = lookup(panel, row_side)
        end = (col_side & 1) ^ flipped
        return panel, side, end + jnp.where(side < 2, 2, 0)

    def cross_col(sheet):
        panel, row_side, col_side = sheet
        panel, side, flipped = lookup(panel, col_side)
        end = (row_side & 1) ^ flipped
        return panel, end + jnp.where(side < 2, 2, 0), side

    for side in range(SIDES):
        panel, other, flipped = lookup(me, side)
        order = jnp.where(flipped == 1, last - lane8, lane8)
        sign = jnp.where(flipped == 1, -1.0, 1.0).astype(F32)
        for field in range(FIELDS):
            values = jnp.take_along_axis(band(panel, other, field), order, axis=1)
            at = (side * FIELDS + field) * DEEP
            parts[at : at + DEEP, :] = values * sign if field == 2 else values

    keys = []
    panels = lax.axis_size("tile") * subs
    for corner, (row_side, col_side) in enumerate(CORNERS):
        start = (me, jnp.int32(row_side), jnp.int32(col_side))
        sheets = {0: start}
        ahead, behind = start, start
        for k in range(DEEP):
            ahead = cross_row(ahead) if k % 2 == 0 else cross_col(ahead)
            behind = cross_col(behind) if k % 2 == 0 else cross_row(behind)
            sheets[k + 1], sheets[-k - 1] = ahead, behind
        sheets[DEEP] = sheets.pop(DEEP)
        filled = [jnp.zeros((DEEP, LANES), F32)] * FIELDS
        key = jnp.full((1, LANES), -1, jnp.int32)
        for k, (panel, side, other) in sheets.items():
            end = other & 1
            order = jnp.where(end == 1, reverse, straight)
            sign = jnp.where(end == 1, -1.0, 1.0).astype(F32)
            if k == DEEP:
                values = roll(jnp.take_along_axis(band(panel, side, 0), order, axis=1), 1, 0)
                filled[0] = jnp.where(far_cell, values, filled[0])
                continue
            here = slot_of == k % SHEETS
            for field in range(FIELDS):
                values = jnp.take_along_axis(band(panel, side, field), order, axis=1)
                values = values * sign if field == 2 else values
                filled[field] = jnp.where(here, values, filled[field])
            if abs(k) <= STEPS:
                key = jnp.where(here[:1], (side * panels + panel) * width + order[:1], key)
        keys.append(key)
        for field in range(FIELDS):
            at = CHAIN_AT + (field * SIDES + corner) * DEEP
            parts[at : at + DEEP, :] = filled[field]
    lane = lane8[:1]
    sides = []
    for side in range(SIDES):
        panel, other, flipped = lookup(me, side)
        sides.append(jnp.where(lane == 0, panel, jnp.where(lane == 1, other, flipped)))
    labels[...] = jnp.concatenate(keys + sides, axis=0).astype(F32)


def gains(levels, slots, count, *refs):
    labels = refs[0]
    records = refs[1 : 1 + count]
    g_main, g_band, g_ew, g_chain, obs, square = refs[1 + count :]
    width = LANES
    last = width - 1
    subs = lax.axis_size("sub")
    me = lax.axis_index("tile") * subs + lax.axis_index("sub")
    panels = lax.axis_size("tile") * subs
    pairs = level_pairs(levels)
    depth_rows = record_rows(levels)
    fold = LANES // slots
    lane_rec = iota((depth_rows, LANES), 1)
    chunks, _, span = obs.shape
    chunk_tiles = span // LANES
    pieces = []
    for ref in records:
        if len(ref.shape) == 3:
            pieces += [ref[index] for index in range(ref.shape[0])]
        else:
            pieces += [ref[at : at + depth_rows, :] for at in range(0, ref.shape[0], depth_rows)]
    for group in range(len(pieces) // fold):
        packed = pieces[group * fold]
        for part in range(1, fold):
            shifted = roll(pieces[group * fold + part], part * slots, 1)
            packed = jnp.where(lane_rec // slots == part, shifted, packed)
        column = (group % chunk_tiles) * LANES
        obs[group // chunk_tiles, :, column : column + LANES] = packed
    label_tall = jnp.concatenate([labels[...], jnp.zeros((LANES - 8, LANES), F32)], axis=0).T
    comps = STEPS * len(pairs)
    partners = []
    for side in range(SIDES):
        row = labels[SIDES + side : SIDES + side + 1, :].astype(jnp.int32)
        partners.append((row[:, 0:1], row[:, 1:2], row[:, 2:3]))

    def hits(mask):
        return jnp.where(mask, 1.0, 0.0).astype(BF16)

    def accumulate(chunk, _):
        data = obs[chunk]
        panel = data[0:1].astype(jnp.int32)
        oi = data[1:2].astype(jnp.int32)
        oj = data[2:3].astype(jnp.int32)
        when = data[3:4].astype(jnp.int32)
        tall = iota((width, span), 0)
        at_row = jnp.where((tall == oi) & (panel == me), 1.0, 0.0)
        half = iota((DEEP, span), 0)
        first_half = half < STEPS
        shallow = half % STEPS
        distance = (oi, last - oi, oj, last - oj)
        pieces = []
        for index in range(len(pairs)):
            g = data[4 + index : 5 + index]
            high = g.astype(BF16).astype(F32)
            pieces.append((high, g - high))
        stacks = [jnp.where(first_half, high, low) for high, low in pieces]

        def product(left, right):
            return lax.dot_general(left, right, NT, preferred_element_type=F32)

        def put(ref, at, value):
            if chunks == 1:
                ref[at] = value
            else:
                ref[at] = ref[at] + value

        at_times = jnp.concatenate([hits((tall == oj) & (when == t + 1)) for t in range(STEPS)], axis=0)
        for index, (high, low) in enumerate(pieces):
            value = product((at_row * high).astype(BF16), at_times) + product((at_row * low).astype(BF16), at_times)
            for t in range(STEPS):
                put(g_main, t * len(pairs) + index, value[:, t * LANES : (t + 1) * LANES])

        def rows_of(depth):
            hit = jnp.where(shallow == depth, 1.0, 0.0)
            return jnp.concatenate(
                [jnp.where(when == t + 1, hit, 0.0) * stack for t in range(STEPS) for stack in stacks], axis=0
            ).astype(BF16)

        def joined(value, comp):
            part = value[comp * DEEP : (comp + 1) * DEEP]
            return part + roll(part, STEPS, 0)

        for side, (q, r, f) in enumerate(partners):
            depth = jnp.where(
                r == 0, distance[0], jnp.where(r == 1, distance[1], jnp.where(r == 2, distance[2], distance[3]))
            )
            along = jnp.where(r < 2, oj, oi)
            along = jnp.where(f == 1, last - along, along)
            value = product(rows_of(jnp.where(panel == q, depth, -1)), hits(tall == along))
            for comp in range(comps):
                if side < 2:
                    put(g_band, (side, comp), joined(value, comp))
                else:
                    put(square, (side - 2, comp), joined(value, comp))
        lefts = jnp.concatenate([rows_of(distance[side]) for side in range(SIDES)], axis=1)
        area = panels * width
        spots = [
            jnp.where(panel < 0, -2, panel * width + (oj if side < 2 else oi) + side * area) for side in range(SIDES)
        ]
        keys = [label_tall[:, corner : corner + 1].astype(jnp.int32) for corner in range(4)]
        for duo in range(2):
            places = jnp.concatenate(
                [
                    jnp.concatenate([hits(keys[corner] == spot) for spot in spots], axis=1)
                    for corner in (2 * duo, 2 * duo + 1)
                ],
                axis=0,
            )
            value = product(lefts, places)
            for comp in range(comps):
                total = joined(value, comp)
                for half_index in range(2):
                    corner = 2 * duo + half_index
                    put(
                        g_chain,
                        (comp, slice(corner * DEEP, (corner + 1) * DEEP)),
                        total[:, half_index * LANES : (half_index + 1) * LANES],
                    )
        return 0

    if chunks == 1:
        accumulate(0, 0)
    else:
        g_main[...] = jnp.zeros(g_main.shape, F32)
        g_band[...] = jnp.zeros(g_band.shape, F32)
        g_chain[...] = jnp.zeros(g_chain.shape, F32)
        square[...] = jnp.zeros(square.shape, F32)
        lax.fori_loop(0, chunks, accumulate, 0)
    for start in range(0, comps, DEEP):
        columns = as_columns([(square[1, comp], square[0, comp]) for comp in range(start, min(comps, start + DEEP))])
        for index, value in enumerate(columns):
            g_ew[start + index] = value


def as_columns(duos):
    groups = [jnp.zeros((DEEP, LANES), F32)] * SHEETS
    for index, (east, west) in enumerate(duos):
        groups[2 * index] = east
        groups[(2 * index - 1) % SHEETS] = jnp.concatenate([west[d : d + 1] for d in reversed(range(DEEP))], axis=0)
    columns = jnp.concatenate(groups, axis=0).T
    return [columns if index == 0 else roll(columns, -2 * DEEP * index, 1) for index in range(len(duos))]


def evolve(levels, *refs):
    scalars, refs = refs[0], refs[1:]
    mix, blend, prior = (
        [scalars[index * levels + level : index * levels + level + 1, :] for level in range(levels)] for index in range(3)
    )
    parts, refs = refs[:levels], refs[levels:]
    fields, refs = refs[:levels], refs[levels:]
    g_main, g_band, g_ew, g_chain = refs[:4]
    image_out, sums_out, x_main, x_ew, w_main, w_ew, f_main, f_ew, images, x_band, w_band, x_chain, w_chain, x_far = refs[4:]
    width = LANES
    pairs = level_pairs(levels)
    inner = slice(EDGE, EDGE + width)
    above, below = slice(EDGE - 1, EDGE), slice(EDGE + width, EDGE + width + 1)
    geometry = Geometry(width)
    for k in range(levels):
        level = rotated(levels, k)
        x_main[0, level, inner] = fields[k][0]
        w_main[level, 0, inner] = fields[k][1]
        w_main[level, 1, inner] = fields[k][2]
        part = parts[k]
        piece = lambda side, field: part[(side * FIELDS + field) * DEEP : (side * FIELDS + field + 1) * DEEP, :]
        for index in range(2):
            x_band[level, index] = piece(index, 0)
            w_band[level, index, 0] = piece(index, 1)
            w_band[level, index, 1] = piece(index, 2)
        columns = as_columns(
            [(piece(3, 0), piece(2, 0)), (piece(3, 2), piece(2, 2)), (piece(3, 1), -piece(2, 1))]
        )
        x_ew[0, level, inner], w_ew[level, 0, inner], w_ew[level, 1, inner] = columns
        chain = lambda field: part[CHAIN_AT + field * SIDES * DEEP : CHAIN_AT + (field + 1) * SIDES * DEEP, :]
        x_chain[level] = chain(0)
        w_chain[level, 0] = chain(1)
        w_chain[level, 1] = chain(2)
        x_far[level] = roll(roll(chain(0), -1, 0), -DEEP, 1)
        w_main[level, 0, above] = -piece(0, 1)[:1]
        w_main[level, 0, below] = piece(1, 1)[:1]
        w_ew[level, 0, above] = -geometry.column_fill(chain(1), NE, NW)
        w_ew[level, 0, below] = geometry.column_fill(chain(1), SE, SW)

    center = [1.0 - 4.0 * mix[level] - 2.0 * blend[level] for level in range(levels)]

    def wind(level, axis, part):
        if part == "c":
            return w_chain[level, axis]
        return w_band[level, 0 if part == "n" else 1, axis]

    def gain(t, low, high, part):
        comp = t * len(pairs) + pairs.index((min(low, high), max(low, high)))
        if part == "c":
            return g_chain[comp]
        return g_band[0 if part == "n" else 1, comp]

    def beside(level):
        return [k for k in (level - 1, level + 1) if 0 <= k < levels]

    def added(terms):
        total = terms[0]
        for term in terms[1:]:
            total = total + term
        return total

    def edges(now, states):
        for level in range(levels):
            state = states[level]
            x_main[now, level, above] = state["n"][:1]
            x_main[now, level, below] = state["s"][:1]
            x_ew[now, level, above] = geometry.column_fill(state["c"], NE, NW)
            x_ew[now, level, below] = geometry.column_fill(state["c"], SE, SW)

    def forward(t, states):
        now, then = t % 2, (t + 1) % 2
        edges(now, states)
        out = []
        for level in range(levels):
            x = states[level]
            top, bottom = x_main[now, level, EDGE : EDGE + 1], x_main[now, level, EDGE + width - 1 : EDGE + width]
            near = geometry.neighbours(x, x, x, x, top, bottom, x_far[level] if t == 0 else None)
            result = {}
            for part in PARTS:
                up, down, west, east = near[part]
                value = center[level] * x[part] + mix[level] * ((up + down) + (west + east))
                value = value + wind(level, 0, part) * (up - down) + wind(level, 1, part) * (west - east)
                for k in beside(level):
                    value = value + blend[level] * states[k][part]
                result[part] = value
            out.append(result)
        for start in range(EDGE, EDGE + width, 8):
            at, before, after = slice(start, start + 8), slice(start - 1, start + 7), slice(start + 1, start + 9)
            mains = [x_main[now, level, at] for level in range(levels)]
            columns = [x_ew[now, level, at] for level in range(levels)]
            fresh = ([], [])
            for level in range(levels):
                lanes = geometry.across((mains[level],) * 2, (columns[level],) * 2)
                for which, (x, w, own) in enumerate(((x_main, w_main, mains), (x_ew, w_ew, columns))):
                    up, down = x[now, level, before], x[now, level, after]
                    west, east = lanes[which]
                    value = center[level] * own[level] + mix[level] * ((up + down) + (west + east))
                    value = value + w[level, 0, at] * (up - down) + w[level, 1, at] * (west - east)
                    if beside(level):
                        value = value + blend[level] * added([own[k] for k in beside(level)])
                    fresh[which].append(value)
            rows = slice(start - EDGE, start - EDGE + 8)
            for which, (x, g, f) in enumerate(((x_main, g_main, f_main), (x_ew, g_ew, f_ew))):
                for level in range(levels):
                    if t < STEPS - 1:
                        x[then, level, at] = fresh[which][level]
                    terms = []
                    for other in range(levels):
                        comp = t * len(pairs) + pairs.index((min(level, other), max(level, other)))
                        terms.append(g[comp, rows] * fresh[which][other])
                    if t < STEPS - 1:
                        f[t, level, rows] = added(terms)
                    else:
                        x[then, level, at] = added(terms)
        forces = [
            {
                part: added([gain(t, level, other, part) * out[other][part] for other in range(levels)])
                for part in PARTS
            }
            for level in range(levels)
        ]
        return out, forces

    def adjoint(t, states, forces):
        now, then = (t + 1) % 2, t % 2
        edges(now, states)
        out = []
        for level in range(levels if forces is not None else 0):
            w = states[level]
            minus0, plus0, minus1, plus1 = {}, {}, {}, {}
            for part in PARTS:
                scaled = mix[level] * w[part]
                p, q = wind(level, 0, part) * w[part], wind(level, 1, part) * w[part]
                minus0[part], plus0[part] = scaled + p, scaled - p
                minus1[part], plus1[part] = scaled + q, scaled - q
            first, final = slice(EDGE, EDGE + 1), slice(EDGE + width - 1, EDGE + width)
            top = (mix[level] + w_main[level, 0, first]) * x_main[now, level, first]
            bottom = (mix[level] - w_main[level, 0, final]) * x_main[now, level, final]
            near = geometry.neighbours(minus0, plus0, minus1, plus1, top, bottom)
            result = {}
            for part in PARTS:
                up, down, west, east = near[part]
                value = center[level] * w[part] + ((up + down) + (west + east)) + forces[level][part]
                for k in beside(level):
                    value = value + blend[k] * states[k][part]
                result[part] = value
            out.append(result)
        for start in range(EDGE, EDGE + width, 8):
            at, before, after = slice(start, start + 8), slice(start - 1, start + 7), slice(start + 1, start + 9)
            rows = slice(start - EDGE, start - EDGE + 8)
            mains = [x_main[now, level, at] for level in range(levels)]
            columns = [x_ew[now, level, at] for level in range(levels)]
            for level in range(levels):
                given = []
                for w, own in ((w_main, mains), (w_ew, columns)):
                    scaled, turned = mix[level] * own[level], w[level, 1, at] * own[level]
                    given.append((scaled - turned, scaled + turned))
                lanes = geometry.across(*given)
                for which, (x, w, own, f) in enumerate(
                    ((x_main, w_main, mains, f_main), (x_ew, w_ew, columns, f_ew))
                ):
                    if which and forces is None:
                        continue
                    up = (mix[level] - w[level, 0, before]) * x[now, level, before]
                    down = (mix[level] + w[level, 0, after]) * x[now, level, after]
                    west, east = lanes[which]
                    value = center[level] * own[level] + ((up + down) + (west + east))
                    for k in beside(level):
                        value = value + blend[k] * own[k]
                    if forces is None:
                        images[level, rows] = value + prior[level] * x_start[level][rows]
                    else:
                        x[then, level, at] = value + f[t - 1, level, rows]
        return out

    x_start = [f_main.at[STEPS - 1, level] for level in range(levels)]
    for level in range(levels):
        x_start[level][...] = x_main[0, level, inner]
    states = [{"n": x_band[k, 0], "s": x_band[k, 1], "c": x_chain[k]} for k in range(levels)]
    forcing = []
    for t in range(STEPS):
        states, forces = forward(t, states)
        forcing.append(forces)
    current = forcing[STEPS - 1]
    for t in range(STEPS - 1, -1, -1):
        current = adjoint(t, current, forcing[t - 1] if t else None)

    zero = jnp.zeros((1, LANES), F32)
    totals = [zero] * 4
    for k in range(levels):
        image = images[rotated(levels, k)]
        residual, direction = fields[k][3], fields[k][0]
        if k == 0:
            image_out[...] = image
        for index, term in enumerate((residual * residual, direction * image, residual * image, image * image)):
            totals[index] = totals[index] + jnp.sum(term, axis=0, keepdims=True)
    sums_out[...] = jnp.concatenate(totals + [zero] * 4, axis=0)


def update(*refs):
    parts = refs[:-7]
    increment, residual, direction, image, increment_new, residual_new, direction_new = refs[-7:]
    total = parts[0][...]
    for part in parts[1:]:
        total = total + part[...]
    total = jnp.sum(total, axis=1, keepdims=True)
    norm_old, curvature, cross, square = (total[index : index + 1] for index in range(4))
    alpha = norm_old / curvature
    norm_new = norm_old - 2.0 * alpha * cross + alpha * alpha * square
    ratio = norm_new / norm_old
    d = direction[...]
    increment_new[...] = increment[...] + alpha * d
    r = residual[...] - alpha * image[...]
    residual_new[...] = r
    direction_new[...] = r + ratio * d


def exchanged(value, axis, mask):
    count = lax.axis_size(axis)
    return lax.ppermute(value, axis, [(i, i ^ mask) for i in range(count)])


def split_exchange(value):
    pairs = [(2 * tile + sub, 2 * (tile ^ (2 + sub)) + sub) for tile in range(4) for sub in range(2)]
    return lax.ppermute(value, ("tile", "sub"), pairs)


def gathered(value, joined):
    tiles, subs = lax.axis_size("tile"), lax.axis_size("sub")
    if tiles > 4:
        return [lax.all_gather(value, ("tile", "sub"), axis=0)]
    if joined:
        out = [value] + [exchanged(value, "tile", mask) for mask in range(1, tiles)]
        whole = jnp.concatenate(out, axis=0)
        return [whole] + [exchanged(whole, "sub", mask) for mask in range(1, subs)]
    out = [value] + [exchanged(value, "sub", mask) for mask in range(1, subs)]
    for mask in range(1, tiles):
        other = exchanged(value, "tile", mask)
        out += [other] + [exchanged(other, "sub", by) for by in range(1, subs)]
    return out


def level_parts(value):
    count = lax.axis_size("lev")
    return [value] + [lax.ppermute(value, "lev", [(i, (i + k) % count) for i in range(count)]) for k in range(1, count)]


def body(
    increment,
    residual,
    direction,
    wind_u,
    wind_v,
    diffusion,
    vertical,
    background_inv,
    side_pair,
    side_flip,
    obs_column,
    obs_time,
    obs_count,
    jacobian,
    error_inv,
):
    width = increment.shape[2]
    slots, _, channels = jacobian.shape
    tiles, subs, levels = lax.axis_size("tile"), lax.axis_size("sub"), lax.axis_size("lev")
    panels = tiles * subs
    shape = (width, width)
    flat = lambda a: a.reshape(shape)
    own = jacobian.reshape(slots, channels)
    depth_rows = record_rows(levels)
    row = lambda a: a.reshape(1, -1)
    scalar_rows = -(-3 * levels // 8) * 8
    bands, fields, wide, places, weights, scalars = pl.pallas_call(
        functools.partial(prepare, width.bit_length() - 1),
        out_shape=(
            pltpu.VMEM((BAND, LANES), F32),
            pltpu.VMEM((4,) + shape, F32),
            pltpu.VMEM((slots, channels), F32),
            pltpu.VMEM((8, LANES), F32),
            pltpu.VMEM((1, channels), F32),
            pltpu.VMEM((scalar_rows, LANES), F32),
        ),
        in_specs=[SCALAR] * 4 + [WHOLE] * 8,
        out_specs=(WHOLE,) * 6,
        compiler_params=limit(60),
        name="prepare",
    )(
        obs_count,
        diffusion,
        vertical,
        background_inv,
        flat(direction),
        flat(wind_u),
        flat(wind_v),
        flat(residual),
        own,
        row(obs_column),
        row(obs_time),
        error_inv,
    )
    all_wide = level_parts(wide)
    all_fields = level_parts(fields)

    record = pl.pallas_call(
        functools.partial(compose, levels),
        out_shape=pltpu.VMEM((depth_rows, LANES), F32),
        in_specs=[WHOLE] * (levels + 2),
        out_specs=WHOLE,
        scratch_shapes=[pltpu.VMEM((levels, slots, channels), F32)],
        compiler_params=limit(8),
        name="compose",
    )(*[near(a) for a in (*all_wide, weights, places)])
    messages, records = gathered(bands, False), gathered(record, True)

    pair, flip = side_pair.T, side_flip.T
    vmem = lambda *dims: pltpu.VMEM(dims, F32)
    parts, labels = pl.pallas_call(
        functools.partial(assemble, len(messages)),
        out_shape=(vmem(CHAIN_AT + FIELDS * SIDES * DEEP, LANES), vmem(8, LANES)),
        in_specs=[SCALAR] * 2 + [WHOLE] * len(messages),
        out_specs=(WHOLE, WHOLE),
        scratch_shapes=[vmem(panels, BAND, LANES)],
        compiler_params=limit(8),
        name="assemble",
    )(pair, flip, *[near(a) for a in messages])
    all_parts = level_parts(parts)

    span = min(CHUNK, panels * slots)
    comps = STEPS * len(level_pairs(levels))
    chain = (SIDES * DEEP, LANES)
    padded = (width + 2 * EDGE, LANES)
    products = pl.pallas_call(
        functools.partial(gains, levels, slots, len(records)),
        out_shape=(vmem(comps, *shape), vmem(2, comps, DEEP, LANES), vmem(comps, *shape), vmem(comps, *chain)),
        in_specs=[WHOLE] * (1 + len(records)),
        out_specs=(WHOLE,) * 4,
        scratch_shapes=[vmem(panels * slots // span, depth_rows, span), vmem(2, comps, DEEP, LANES)],
        compiler_params=limit(16),
        name="gains",
    )(*[near(a) for a in (labels, *records)])

    image, sums = pl.pallas_call(
        functools.partial(evolve, levels),
        out_shape=(vmem(*shape), vmem(8, LANES)),
        in_specs=[WHOLE] * (2 * levels + 5),
        out_specs=(WHOLE, WHOLE),
        scratch_shapes=[
            vmem(2, levels, *padded),
            vmem(2, levels, *padded),
            vmem(levels, 2, *padded),
            vmem(levels, 2, *padded),
            vmem(STEPS, levels, *shape),
            vmem(STEPS, levels, *shape),
            vmem(levels, *shape),
            vmem(levels, 2, DEEP, LANES),
            vmem(levels, 2, 2, DEEP, LANES),
            vmem(levels, *chain),
            vmem(levels, 2, *chain),
            vmem(levels, *chain),
        ],
        compiler_params=limit(12),
        name="evolve",
    )(*[near(a) for a in (scalars, *all_parts, *all_fields, *products)])

    for mask in range(1, subs):
        sums = sums + exchanged(sums, "sub", mask)
    if (tiles, subs) == (4, 2):
        far = split_exchange(sums)
        parts = [sums, far, exchanged(sums, "tile", 1), exchanged(far, "sub", 1)]
    else:
        mask = 1
        while mask < tiles:
            sums = sums + exchanged(sums, "tile", mask)
            mask *= 2
        parts = [sums]
    outputs = pl.pallas_call(
        update,
        out_shape=(jax.ShapeDtypeStruct(shape, F32),) * 3,
        in_specs=[WHOLE] * (len(parts) + 4),
        out_specs=(WHOLE,) * 3,
        compiler_params=limit(4),
        name="update",
    )(*[near(a) for a in (*parts, flat(increment), flat(residual), flat(direction), image)])
    return tuple(out.reshape(increment.shape) for out in outputs)


def solution(mesh):
    field = P(("member", "lev"), ("tile", "sub"), None)
    placed = (
        (field,) * 5
        + (P(),) * 5
        + (P(("tile", "sub")),) * 3
        + (P(("tile", "sub"), "lev", None), P())
    )
    return jax.shard_map(body, mesh=mesh, in_specs=placed, out_specs=(field,) * 3, check_vma=False)
```

```python
import functools

import jax
import jax.numpy as jnp
from jax import lax
from jax.experimental import pallas as pl
from jax.experimental.pallas import tpu as pltpu
from jax.sharding import PartitionSpec as P


STEPS = 4
DEEP = 2 * STEPS
SIDES = 4
FIELDS = 3
BAND = SIDES * FIELDS * DEEP
LANES = 128
CHAIN_AT = BAND
SHEETS = LANES // DEEP
CHUNK = 512
F32 = jnp.float32
BF16 = jnp.bfloat16
NT = (((1,), (1,)), ((), ()))
WHOLE = pl.BlockSpec(memory_space=pltpu.VMEM)
SCALAR = pl.BlockSpec(memory_space=pltpu.SMEM)
CORNERS = ((0, 2), (0, 3), (1, 2), (1, 3))
NW, NE, SW, SE = range(4)


def near(value):
    return pltpu.with_memory_space_constraint(value, pltpu.VMEM)


def limit(mebibytes):
    return pltpu.CompilerParams(vmem_limit_bytes=mebibytes << 20)


def iota(shape, axis):
    return lax.broadcasted_iota(jnp.int32, shape, axis)


def level_pairs(levels):
    return [(low, high) for low in range(levels) for high in range(low, levels)]


def record_rows(levels):
    return -(-(4 + len(level_pairs(levels))) // 8) * 8


def rotated(levels, k):
    return lax.rem(lax.axis_index("lev") + (levels - k), levels)


def prepare(bits, count, diffusion, vertical, prior, direction, wind_u, wind_v, residual, jacobian, columns, times, errors, bands, fields, wide, places, weights, scalars):
    x = direction[...]
    u = 0.5 * wind_u[...].astype(F32)
    v = 0.5 * wind_v[...].astype(F32)
    width = x.shape[0]
    wide[...] = jacobian[...].astype(F32)
    fields[0] = x
    fields[1] = u
    fields[2] = v
    fields[3] = residual[...]
    slots = columns.shape[1]
    column = columns[...]
    mask = (1 << bits) - 1
    alive = iota((1, slots), 1) < count[0]
    panel = jnp.where(alive, lax.shift_right_logical(column, 2 * bits), -1)
    rows = [panel, lax.shift_right_logical(column, bits) & mask, column & mask, times[...]]
    rows = jnp.concatenate(rows + rows, axis=0).astype(F32)
    if slots < LANES:
        rows = jnp.concatenate([rows, jnp.full((rows.shape[0], LANES - slots), -1.0, F32)], axis=1)
    places[...] = rows
    weights[...] = errors[...].reshape(1, -1)
    levels = diffusion.shape[0]
    scalars[...] = jnp.zeros(scalars.shape, F32)
    for index, values in enumerate((diffusion, vertical, prior)):
        for level in range(levels):
            at = index * levels + level
            scalars[at : at + 1, :] = jnp.full((1, LANES), values[level], F32)
    first = lambda a: a[:DEEP]
    last = lambda a: jnp.concatenate([a[width - 1 - d : width - d] for d in range(DEEP)], axis=0)
    xt, ut, vt = x.T, u.T, v.T
    parts = [
        (first(x), first(u), first(v)),
        (last(x), -last(u), last(v)),
        (first(xt), first(vt), first(ut)),
        (last(xt), -last(vt), last(ut)),
    ]
    for side in range(SIDES):
        for field in range(FIELDS):
            row = (side * FIELDS + field) * DEEP
            bands[row : row + DEEP, :] = parts[side][field]


def compose(levels, *refs):
    jacobians = refs[:levels]
    weights, places, record, ordered = refs[levels:]
    for k in range(levels):
        ordered[rotated(levels, k)] = jacobians[k][...]
    slots = ordered.shape[1]
    ones = jnp.ones((8, ordered.shape[2]), F32)
    scale = weights[...]
    rows = []
    pairs = level_pairs(levels)
    stacked = jnp.concatenate([ordered[low] * scale * ordered[high] for low, high in pairs], axis=0)
    totals = lax.dot_general(ones, stacked, NT, precision=lax.Precision.HIGHEST, preferred_element_type=F32)
    rows += [totals[:1, index * slots : (index + 1) * slots] for index in range(len(pairs))]
    spare = record_rows(levels) - 4 - len(rows)
    if spare:
        rows.append(jnp.zeros((spare, slots), F32))
    whole = jnp.concatenate(rows, axis=0)
    if slots < LANES:
        whole = jnp.concatenate([whole, jnp.zeros((whole.shape[0], LANES - slots), F32)], axis=1)
    record[...] = jnp.concatenate([places[:4, :], whole], axis=0)


def roll(a, shift, axis):
    return pltpu.roll(a, shift % a.shape[axis], axis)


class Geometry:
    def __init__(self, width):
        self.last = last = width - 1
        row, lane = iota((DEEP, LANES), 0), iota((DEEP, LANES), 1)
        self.band_first = row == 0
        self.left, self.right = lane == 0, lane == last
        self.near = lane < LANES // 2
        self.mirror = jnp.where(lane >= LANES - DEEP, 2 * LANES - 2 * DEEP + last - LANES - lane, lane)
        crow, clane = iota((SIDES * DEEP, LANES), 0), iota((SIDES * DEEP, LANES), 1)
        self.chain_top = crow % DEEP == 0
        self.chain_left = clane % DEEP == 0
        self.even = (clane // DEEP) % 2 == 0
        self.seventh = clane // DEEP == DEEP - 1

    def chain(self, a, corner):
        return a[corner * DEEP : (corner + 1) * DEEP]

    def band_west(self, a, chain_block):
        return jnp.where(self.left, roll(chain_block, -2 * DEEP, 1), roll(a, 1, 1))

    def band_east(self, a, chain_block):
        return jnp.where(self.right, roll(chain_block, self.last - 2 * DEEP, 1), roll(a, -1, 1))

    def column_fill(self, a, east, west):
        mirrored = jnp.take_along_axis(self.chain(a, west), self.mirror, axis=1)
        return jnp.where(self.near, roll(self.chain(a, east), 2 * DEEP, 1), mirrored)[:1]

    def chain_up(self, a, fill):
        swapped = jnp.where(self.even, roll(fill, -DEEP, 1), roll(fill, DEEP, 1))
        return jnp.where(self.chain_top, swapped, roll(a, 1, 0))

    def chain_west(self, a, fill, beyond=None):
        swapped = jnp.where(self.even, roll(fill, DEEP, 1), roll(fill, -DEEP, 1))
        if beyond is not None:
            swapped = jnp.where(self.seventh, beyond, swapped)
        return jnp.where(self.chain_left, swapped, roll(a, 1, 1))

    def across(self, main, columns):
        before_m, before_c = roll(main[0], 1, 1), roll(columns[0], 1, 1)
        after_m, after_c = roll(main[1], -1, 1), roll(columns[1], -1, 1)
        left, right = self.left, self.right
        return (
            (jnp.where(left, before_c, before_m), jnp.where(right, after_c, after_m)),
            (jnp.where(left, before_m, before_c), jnp.where(right, after_m, after_c)),
        )

    def neighbours(self, minus0, plus0, minus1, plus1, top, bottom, beyond=None):
        out = {}
        for part, row, west, east in (("n", top, NW, NE), ("s", bottom, SW, SE)):
            out[part] = (
                jnp.where(self.band_first, row, roll(plus0[part], 1, 0)),
                roll(minus0[part], -1, 0),
                self.band_west(plus1[part], self.chain(minus1["c"], west)),
                self.band_east(minus1[part], self.chain(minus1["c"], east)),
            )
        out["c"] = (
            self.chain_up(plus0["c"], minus0["c"]),
            roll(minus0["c"], -1, 0),
            self.chain_west(plus1["c"], minus1["c"], beyond),
            roll(minus1["c"], -1, 1),
        )
        return out


PARTS = ("n", "s", "c")
EDGE = 8


def assemble(count, *refs):
    pair, flip = refs[:2]
    messages = refs[2 : 2 + count]
    parts, labels, table = refs[2 + count :]
    width = LANES
    last = width - 1
    subs = lax.axis_size("sub")
    tile, sub = lax.axis_index("tile"), lax.axis_index("sub")
    me = tile * subs + sub
    if count == 1:
        source = messages[0]
    else:
        source = table
        for index in range(count):
            xt, xs = index // subs, index % subs
            table[(tile ^ xt) * subs + (sub ^ xs)] = messages[index][...]

    lane8 = iota((DEEP, LANES), 1)
    straight, reverse = lane8 % DEEP, last - lane8 % DEEP
    slot_of = lane8 // DEEP
    far_cell = (lane8 == DEEP * DEEP) & (iota((DEEP, LANES), 0) == 1)

    def band(panel, side, field):
        start = pl.multiple_of((side * FIELDS + field) * DEEP, 8)
        return source[panel, pl.ds(start, DEEP), :]

    def lookup(panel, side):
        other = pair[side, panel]
        return lax.shift_right_logical(other, 2), other & 3, flip[side, panel]

    def cross_row(sheet):
        panel, row_side, col_side = sheet
        panel, side, flipped = lookup(panel, row_side)
        end = (col_side & 1) ^ flipped
        return panel, side, end + jnp.where(side < 2, 2, 0)

    def cross_col(sheet):
        panel, row_side, col_side = sheet
        panel, side, flipped = lookup(panel, col_side)
        end = (row_side & 1) ^ flipped
        return panel, end + jnp.where(side < 2, 2, 0), side

    for side in range(SIDES):
        panel, other, flipped = lookup(me, side)
        order = jnp.where(flipped == 1, last - lane8, lane8)
        sign = jnp.where(flipped == 1, -1.0, 1.0).astype(F32)
        for field in range(FIELDS):
            values = jnp.take_along_axis(band(panel, other, field), order, axis=1)
            at = (side * FIELDS + field) * DEEP
            parts[at : at + DEEP, :] = values * sign if field == 2 else values

    keys = []
    panels = lax.axis_size("tile") * subs
    for corner, (row_side, col_side) in enumerate(CORNERS):
        start = (me, jnp.int32(row_side), jnp.int32(col_side))
        sheets = {0: start}
        ahead, behind = start, start
        for k in range(DEEP):
            ahead = cross_row(ahead) if k % 2 == 0 else cross_col(ahead)
            behind = cross_col(behind) if k % 2 == 0 else cross_row(behind)
            sheets[k + 1], sheets[-k - 1] = ahead, behind
        sheets[DEEP] = sheets.pop(DEEP)
        filled = [jnp.zeros((DEEP, LANES), F32)] * FIELDS
        key = jnp.full((1, LANES), -1, jnp.int32)
        for k, (panel, side, other) in sheets.items():
            end = other & 1
            order = jnp.where(end == 1, reverse, straight)
            sign = jnp.where(end == 1, -1.0, 1.0).astype(F32)
            if k == DEEP:
                values = roll(jnp.take_along_axis(band(panel, side, 0), order, axis=1), 1, 0)
                filled[0] = jnp.where(far_cell, values, filled[0])
                continue
            here = slot_of == k % SHEETS
            for field in range(FIELDS):
                values = jnp.take_along_axis(band(panel, side, field), order, axis=1)
                values = values * sign if field == 2 else values
                filled[field] = jnp.where(here, values, filled[field])
            if abs(k) <= STEPS:
                key = jnp.where(here[:1], (side * panels + panel) * width + order[:1], key)
        keys.append(key)
        for field in range(FIELDS):
            at = CHAIN_AT + (field * SIDES + corner) * DEEP
            parts[at : at + DEEP, :] = filled[field]
    lane = lane8[:1]
    sides = []
    for side in range(SIDES):
        panel, other, flipped = lookup(me, side)
        sides.append(jnp.where(lane == 0, panel, jnp.where(lane == 1, other, flipped)))
    labels[...] = jnp.concatenate(keys + sides, axis=0).astype(F32)


def gains(levels, slots, count, *refs):
    labels = refs[0]
    records = refs[1 : 1 + count]
    g_main, g_band, g_ew, g_chain, obs, square = refs[1 + count :]
    width = LANES
    last = width - 1
    subs = lax.axis_size("sub")
    me = lax.axis_index("tile") * subs + lax.axis_index("sub")
    panels = lax.axis_size("tile") * subs
    pairs = level_pairs(levels)
    depth_rows = record_rows(levels)
    fold = LANES // slots
    lane_rec = iota((depth_rows, LANES), 1)
    chunks, _, span = obs.shape
    chunk_tiles = span // LANES
    pieces = []
    for ref in records:
        if len(ref.shape) == 3:
            pieces += [ref[index] for index in range(ref.shape[0])]
        else:
            pieces += [ref[at : at + depth_rows, :] for at in range(0, ref.shape[0], depth_rows)]
    for group in range(len(pieces) // fold):
        packed = pieces[group * fold]
        for part in range(1, fold):
            shifted = roll(pieces[group * fold + part], part * slots, 1)
            packed = jnp.where(lane_rec // slots == part, shifted, packed)
        column = (group % chunk_tiles) * LANES
        obs[group // chunk_tiles, :, column : column + LANES] = packed
    label_tall = jnp.concatenate([labels[...], jnp.zeros((LANES - 8, LANES), F32)], axis=0).T
    comps = STEPS * len(pairs)
    partners = []
    for side in range(SIDES):
        row = labels[SIDES + side : SIDES + side + 1, :].astype(jnp.int32)
        partners.append((row[:, 0:1], row[:, 1:2], row[:, 2:3]))

    def hits(mask):
        return jnp.where(mask, 1.0, 0.0).astype(BF16)

    def accumulate(chunk, _):
        data = obs[chunk]
        panel = data[0:1].astype(jnp.int32)
        oi = data[1:2].astype(jnp.int32)
        oj = data[2:3].astype(jnp.int32)
        when = data[3:4].astype(jnp.int32)
        tall = iota((width, span), 0)
        at_row = jnp.where((tall == oi) & (panel == me), 1.0, 0.0)
        half = iota((DEEP, span), 0)
        first_half = half < STEPS
        shallow = half % STEPS
        distance = (oi, last - oi, oj, last - oj)
        pieces = []
        for index in range(len(pairs)):
            g = data[4 + index : 5 + index]
            high = g.astype(BF16).astype(F32)
            pieces.append((high, g - high))
        stacks = [jnp.where(first_half, high, low) for high, low in pieces]

        def product(left, right):
            return lax.dot_general(left, right, NT, preferred_element_type=F32)

        def put(ref, at, value):
            if chunks == 1:
                ref[at] = value
            else:
                ref[at] = ref[at] + value

        at_times = jnp.concatenate([hits((tall == oj) & (when == t + 1)) for t in range(STEPS)], axis=0)
        for index, (high, low) in enumerate(pieces):
            value = product((at_row * high).astype(BF16), at_times) + product((at_row * low).astype(BF16), at_times)
            for t in range(STEPS):
                put(g_main, t * len(pairs) + index, value[:, t * LANES : (t + 1) * LANES])

        def rows_of(depth):
            hit = jnp.where(shallow == depth, 1.0, 0.0)
            return jnp.concatenate(
                [jnp.where(when == t + 1, hit, 0.0) * stack for t in range(STEPS) for stack in stacks], axis=0
            ).astype(BF16)

        def joined(value, comp):
            part = value[comp * DEEP : (comp + 1) * DEEP]
            return part + roll(part, STEPS, 0)

        for side, (q, r, f) in enumerate(partners):
            depth = jnp.where(
                r == 0, distance[0], jnp.where(r == 1, distance[1], jnp.where(r == 2, distance[2], distance[3]))
            )
            along = jnp.where(r < 2, oj, oi)
            along = jnp.where(f == 1, last - along, along)
            value = product(rows_of(jnp.where(panel == q, depth, -1)), hits(tall == along))
            for comp in range(comps):
                if side < 2:
                    put(g_band, (side, comp), joined(value, comp))
                else:
                    put(square, (side - 2, comp), joined(value, comp))
        lefts = jnp.concatenate([rows_of(distance[side]) for side in range(SIDES)], axis=1)
        area = panels * width
        spots = [
            jnp.where(panel < 0, -2, panel * width + (oj if side < 2 else oi) + side * area) for side in range(SIDES)
        ]
        keys = [label_tall[:, corner : corner + 1].astype(jnp.int32) for corner in range(4)]
        for duo in range(2):
            places = jnp.concatenate(
                [
                    jnp.concatenate([hits(keys[corner] == spot) for spot in spots], axis=1)
                    for corner in (2 * duo, 2 * duo + 1)
                ],
                axis=0,
            )
            value = product(lefts, places)
            for comp in range(comps):
                total = joined(value, comp)
                for half_index in range(2):
                    corner = 2 * duo + half_index
                    put(
                        g_chain,
                        (comp, slice(corner * DEEP, (corner + 1) * DEEP)),
                        total[:, half_index * LANES : (half_index + 1) * LANES],
                    )
        return 0

    if chunks == 1:
        accumulate(0, 0)
    else:
        g_main[...] = jnp.zeros(g_main.shape, F32)
        g_band[...] = jnp.zeros(g_band.shape, F32)
        g_chain[...] = jnp.zeros(g_chain.shape, F32)
        square[...] = jnp.zeros(square.shape, F32)
        lax.fori_loop(0, chunks, accumulate, 0)
    for start in range(0, comps, DEEP):
        columns = as_columns([(square[1, comp], square[0, comp]) for comp in range(start, min(comps, start + DEEP))])
        for index, value in enumerate(columns):
            g_ew[start + index] = value


def as_columns(duos):
    groups = [jnp.zeros((DEEP, LANES), F32)] * SHEETS
    for index, (east, west) in enumerate(duos):
        groups[2 * index] = east
        groups[(2 * index - 1) % SHEETS] = jnp.concatenate([west[d : d + 1] for d in reversed(range(DEEP))], axis=0)
    columns = jnp.concatenate(groups, axis=0).T
    return [columns if index == 0 else roll(columns, -2 * DEEP * index, 1) for index in range(len(duos))]


def evolve(levels, *refs):
    scalars, refs = refs[0], refs[1:]
    mix, blend, prior = (
        [scalars[index * levels + level : index * levels + level + 1, :] for level in range(levels)] for index in range(3)
    )
    parts, refs = refs[:levels], refs[levels:]
    fields, refs = refs[:levels], refs[levels:]
    g_main, g_band, g_ew, g_chain = refs[:4]
    image_out, sums_out, x_main, x_ew, w_main, w_ew, f_main, f_ew, images, x_band, w_band, x_chain, w_chain, x_far = refs[4:]
    width = LANES
    pairs = level_pairs(levels)
    inner = slice(EDGE, EDGE + width)
    above, below = slice(EDGE - 1, EDGE), slice(EDGE + width, EDGE + width + 1)
    geometry = Geometry(width)
    for k in range(levels):
        level = rotated(levels, k)
        x_main[0, level, inner] = fields[k][0]
        w_main[level, 0, inner] = fields[k][1]
        w_main[level, 1, inner] = fields[k][2]
        part = parts[k]
        piece = lambda side, field: part[(side * FIELDS + field) * DEEP : (side * FIELDS + field + 1) * DEEP, :]
        for index in range(2):
            x_band[level, index] = piece(index, 0)
            w_band[level, index, 0] = piece(index, 1)
            w_band[level, index, 1] = piece(index, 2)
        columns = as_columns(
            [(piece(3, 0), piece(2, 0)), (piece(3, 2), piece(2, 2)), (piece(3, 1), -piece(2, 1))]
        )
        x_ew[0, level, inner], w_ew[level, 0, inner], w_ew[level, 1, inner] = columns
        chain = lambda field: part[CHAIN_AT + field * SIDES * DEEP : CHAIN_AT + (field + 1) * SIDES * DEEP, :]
        x_chain[level] = chain(0)
        w_chain[level, 0] = chain(1)
        w_chain[level, 1] = chain(2)
        x_far[level] = roll(roll(chain(0), -1, 0), -DEEP, 1)
        w_main[level, 0, above] = -piece(0, 1)[:1]
        w_main[level, 0, below] = piece(1, 1)[:1]
        w_ew[level, 0, above] = -geometry.column_fill(chain(1), NE, NW)
        w_ew[level, 0, below] = geometry.column_fill(chain(1), SE, SW)

    center = [1.0 - 4.0 * mix[level] - 2.0 * blend[level] for level in range(levels)]

    def wind(level, axis, part):
        if part == "c":
            return w_chain[level, axis]
        return w_band[level, 0 if part == "n" else 1, axis]

    def gain(t, low, high, part):
        comp = t * len(pairs) + pairs.index((min(low, high), max(low, high)))
        if part == "c":
            return g_chain[comp]
        return g_band[0 if part == "n" else 1, comp]

    def beside(level):
        return [k for k in (level - 1, level + 1) if 0 <= k < levels]

    def added(terms):
        total = terms[0]
        for term in terms[1:]:
            total = total + term
        return total

    def edges(now, states):
        for level in range(levels):
            state = states[level]
            x_main[now, level, above] = state["n"][:1]
            x_main[now, level, below] = state["s"][:1]
            x_ew[now, level, above] = geometry.column_fill(state["c"], NE, NW)
            x_ew[now, level, below] = geometry.column_fill(state["c"], SE, SW)

    def forward(t, states):
        now, then = t % 2, (t + 1) % 2
        edges(now, states)
        out = []
        for level in range(levels):
            x = states[level]
            top, bottom = x_main[now, level, EDGE : EDGE + 1], x_main[now, level, EDGE + width - 1 : EDGE + width]
            near = geometry.neighbours(x, x, x, x, top, bottom, x_far[level] if t == 0 else None)
            result = {}
            for part in PARTS:
                up, down, west, east = near[part]
                value = center[level] * x[part] + mix[level] * ((up + down) + (west + east))
                value = value + wind(level, 0, part) * (up - down) + wind(level, 1, part) * (west - east)
                for k in beside(level):
                    value = value + blend[level] * states[k][part]
                result[part] = value
            out.append(result)
        for start in range(EDGE, EDGE + width, 8):
            at, before, after = slice(start, start + 8), slice(start - 1, start + 7), slice(start + 1, start + 9)
            mains = [x_main[now, level, at] for level in range(levels)]
            columns = [x_ew[now, level, at] for level in range(levels)]
            fresh = ([], [])
            for level in range(levels):
                lanes = geometry.across((mains[level],) * 2, (columns[level],) * 2)
                for which, (x, w, own) in enumerate(((x_main, w_main, mains), (x_ew, w_ew, columns))):
                    up, down = x[now, level, before], x[now, level, after]
                    west, east = lanes[which]
                    value = center[level] * own[level] + mix[level] * ((up + down) + (west + east))
                    value = value + w[level, 0, at] * (up - down) + w[level, 1, at] * (west - east)
                    if beside(level):
                        value = value + blend[level] * added([own[k] for k in beside(level)])
                    fresh[which].append(value)
            rows = slice(start - EDGE, start - EDGE + 8)
            for which, (x, g, f) in enumerate(((x_main, g_main, f_main), (x_ew, g_ew, f_ew))):
                for level in range(levels):
                    if t < STEPS - 1:
                        x[then, level, at] = fresh[which][level]
                    terms = []
                    for other in range(levels):
                        comp = t * len(pairs) + pairs.index((min(level, other), max(level, other)))
                        terms.append(g[comp, rows] * fresh[which][other])
                    if t < STEPS - 1:
                        f[t, level, rows] = added(terms)
                    else:
                        x[then, level, at] = added(terms)
        forces = [
            {
                part: added([gain(t, level, other, part) * out[other][part] for other in range(levels)])
                for part in PARTS
            }
            for level in range(levels)
        ]
        return out, forces

    def adjoint(t, states, forces):
        now, then = (t + 1) % 2, t % 2
        edges(now, states)
        out = []
        for level in range(levels if forces is not None else 0):
            w = states[level]
            minus0, plus0, minus1, plus1 = {}, {}, {}, {}
            for part in PARTS:
                scaled = mix[level] * w[part]
                p, q = wind(level, 0, part) * w[part], wind(level, 1, part) * w[part]
                minus0[part], plus0[part] = scaled + p, scaled - p
                minus1[part], plus1[part] = scaled + q, scaled - q
            first, final = slice(EDGE, EDGE + 1), slice(EDGE + width - 1, EDGE + width)
            top = (mix[level] + w_main[level, 0, first]) * x_main[now, level, first]
            bottom = (mix[level] - w_main[level, 0, final]) * x_main[now, level, final]
            near = geometry.neighbours(minus0, plus0, minus1, plus1, top, bottom)
            result = {}
            for part in PARTS:
                up, down, west, east = near[part]
                value = center[level] * w[part] + ((up + down) + (west + east)) + forces[level][part]
                for k in beside(level):
                    value = value + blend[k] * states[k][part]
                result[part] = value
            out.append(result)
        for start in range(EDGE, EDGE + width, 8):
            at, before, after = slice(start, start + 8), slice(start - 1, start + 7), slice(start + 1, start + 9)
            rows = slice(start - EDGE, start - EDGE + 8)
            mains = [x_main[now, level, at] for level in range(levels)]
            columns = [x_ew[now, level, at] for level in range(levels)]
            for level in range(levels):
                given = []
                for w, own in ((w_main, mains), (w_ew, columns)):
                    scaled, turned = mix[level] * own[level], w[level, 1, at] * own[level]
                    given.append((scaled - turned, scaled + turned))
                lanes = geometry.across(*given)
                for which, (x, w, own, f) in enumerate(
                    ((x_main, w_main, mains, f_main), (x_ew, w_ew, columns, f_ew))
                ):
                    if which and forces is None:
                        continue
                    up = (mix[level] - w[level, 0, before]) * x[now, level, before]
                    down = (mix[level] + w[level, 0, after]) * x[now, level, after]
                    west, east = lanes[which]
                    value = center[level] * own[level] + ((up + down) + (west + east))
                    for k in beside(level):
                        value = value + blend[k] * own[k]
                    if forces is None:
                        images[level, rows] = value + prior[level] * x_start[level][rows]
                    else:
                        x[then, level, at] = value + f[t - 1, level, rows]
        return out

    x_start = [f_main.at[STEPS - 1, level] for level in range(levels)]
    for level in range(levels):
        x_start[level][...] = x_main[0, level, inner]
    states = [{"n": x_band[k, 0], "s": x_band[k, 1], "c": x_chain[k]} for k in range(levels)]
    forcing = []
    for t in range(STEPS):
        states, forces = forward(t, states)
        forcing.append(forces)
    current = forcing[STEPS - 1]
    for t in range(STEPS - 1, -1, -1):
        current = adjoint(t, current, forcing[t - 1] if t else None)

    zero = jnp.zeros((1, LANES), F32)
    totals = [zero] * 4
    for k in range(levels):
        image = images[rotated(levels, k)]
        residual, direction = fields[k][3], fields[k][0]
        if k == 0:
            image_out[...] = image
        for index, term in enumerate((residual * residual, direction * image, residual * image, image * image)):
            totals[index] = totals[index] + jnp.sum(term, axis=0, keepdims=True)
    sums_out[...] = jnp.concatenate(totals + [zero] * 4, axis=0)


def update(*refs):
    parts = refs[:-7]
    increment, residual, direction, image, increment_new, residual_new, direction_new = refs[-7:]
    total = parts[0][...]
    for part in parts[1:]:
        total = total + part[...]
    total = jnp.sum(total, axis=1, keepdims=True)
    norm_old, curvature, cross, square = (total[index : index + 1] for index in range(4))
    alpha = norm_old / curvature
    norm_new = norm_old - 2.0 * alpha * cross + alpha * alpha * square
    ratio = norm_new / norm_old
    d = direction[...]
    increment_new[...] = increment[...] + alpha * d
    r = residual[...] - alpha * image[...]
    residual_new[...] = r
    direction_new[...] = r + ratio * d


def exchanged(value, axis, mask):
    count = lax.axis_size(axis)
    return lax.ppermute(value, axis, [(i, i ^ mask) for i in range(count)])


def split_exchange(value):
    pairs = [(2 * tile + sub, 2 * (tile ^ (2 + sub)) + sub) for tile in range(4) for sub in range(2)]
    return lax.ppermute(value, ("tile", "sub"), pairs)


def gathered(value, joined):
    tiles, subs = lax.axis_size("tile"), lax.axis_size("sub")
    if tiles > 4:
        return [lax.all_gather(value, ("tile", "sub"), axis=0)]
    if joined:
        out = [value] + [exchanged(value, "tile", mask) for mask in range(1, tiles)]
        whole = jnp.concatenate(out, axis=0)
        return [whole] + [exchanged(whole, "sub", mask) for mask in range(1, subs)]
    out = [value] + [exchanged(value, "sub", mask) for mask in range(1, subs)]
    for mask in range(1, tiles):
        other = exchanged(value, "tile", mask)
        out += [other] + [exchanged(other, "sub", by) for by in range(1, subs)]
    return out


def level_parts(value):
    count = lax.axis_size("lev")
    return [value] + [lax.ppermute(value, "lev", [(i, (i + k) % count) for i in range(count)]) for k in range(1, count)]


def body(
    increment,
    residual,
    direction,
    wind_u,
    wind_v,
    diffusion,
    vertical,
    background_inv,
    side_pair,
    side_flip,
    obs_column,
    obs_time,
    obs_count,
    jacobian,
    error_inv,
):
    width = increment.shape[2]
    slots, _, channels = jacobian.shape
    tiles, subs, levels = lax.axis_size("tile"), lax.axis_size("sub"), lax.axis_size("lev")
    panels = tiles * subs
    shape = (width, width)
    flat = lambda a: a.reshape(shape)
    own = jacobian.reshape(slots, channels)
    depth_rows = record_rows(levels)
    row = lambda a: a.reshape(1, -1)
    scalar_rows = -(-3 * levels // 8) * 8
    bands, fields, wide, places, weights, scalars = pl.pallas_call(
        functools.partial(prepare, width.bit_length() - 1),
        out_shape=(
            pltpu.VMEM((BAND, LANES), F32),
            pltpu.VMEM((4,) + shape, F32),
            pltpu.VMEM((slots, channels), F32),
            pltpu.VMEM((8, LANES), F32),
            pltpu.VMEM((1, channels), F32),
            pltpu.VMEM((scalar_rows, LANES), F32),
        ),
        in_specs=[SCALAR] * 4 + [WHOLE] * 8,
        out_specs=(WHOLE,) * 6,
        compiler_params=limit(60),
        name="prepare",
    )(
        obs_count,
        diffusion,
        vertical,
        background_inv,
        flat(direction),
        flat(wind_u),
        flat(wind_v),
        flat(residual),
        own,
        row(obs_column),
        row(obs_time),
        error_inv,
    )
    all_wide = level_parts(wide)
    all_fields = level_parts(fields)

    record = pl.pallas_call(
        functools.partial(compose, levels),
        out_shape=pltpu.VMEM((depth_rows, LANES), F32),
        in_specs=[WHOLE] * (levels + 2),
        out_specs=WHOLE,
        scratch_shapes=[pltpu.VMEM((levels, slots, channels), F32)],
        compiler_params=limit(8),
        name="compose",
    )(*[near(a) for a in (*all_wide, weights, places)])
    messages, records = gathered(bands, False), gathered(record, True)

    pair, flip = side_pair.T, side_flip.T
    vmem = lambda *dims: pltpu.VMEM(dims, F32)
    parts, labels = pl.pallas_call(
        functools.partial(assemble, len(messages)),
        out_shape=(vmem(CHAIN_AT + FIELDS * SIDES * DEEP, LANES), vmem(8, LANES)),
        in_specs=[SCALAR] * 2 + [WHOLE] * len(messages),
        out_specs=(WHOLE, WHOLE),
        scratch_shapes=[vmem(panels, BAND, LANES)],
        compiler_params=limit(8),
        name="assemble",
    )(pair, flip, *[near(a) for a in messages])
    all_parts = level_parts(parts)

    span = min(CHUNK, panels * slots)
    comps = STEPS * len(level_pairs(levels))
    chain = (SIDES * DEEP, LANES)
    padded = (width + 2 * EDGE, LANES)
    products = pl.pallas_call(
        functools.partial(gains, levels, slots, len(records)),
        out_shape=(vmem(comps, *shape), vmem(2, comps, DEEP, LANES), vmem(comps, *shape), vmem(comps, *chain)),
        in_specs=[WHOLE] * (1 + len(records)),
        out_specs=(WHOLE,) * 4,
        scratch_shapes=[vmem(panels * slots // span, depth_rows, span), vmem(2, comps, DEEP, LANES)],
        compiler_params=limit(16),
        name="gains",
    )(*[near(a) for a in (labels, *records)])

    image, sums = pl.pallas_call(
        functools.partial(evolve, levels),
        out_shape=(vmem(*shape), vmem(8, LANES)),
        in_specs=[WHOLE] * (2 * levels + 5),
        out_specs=(WHOLE, WHOLE),
        scratch_shapes=[
            vmem(2, levels, *padded),
            vmem(2, levels, *padded),
            vmem(levels, 2, *padded),
            vmem(levels, 2, *padded),
            vmem(STEPS, levels, *shape),
            vmem(STEPS, levels, *shape),
            vmem(levels, *shape),
            vmem(levels, 2, DEEP, LANES),
            vmem(levels, 2, 2, DEEP, LANES),
            vmem(levels, *chain),
            vmem(levels, 2, *chain),
            vmem(levels, *chain),
        ],
        compiler_params=limit(12),
        name="evolve",
    )(*[near(a) for a in (scalars, *all_parts, *all_fields, *products)])

    for mask in range(1, subs):
        sums = sums + exchanged(sums, "sub", mask)
    if (tiles, subs) == (4, 2):
        far = split_exchange(sums)
        parts = [sums, far, exchanged(sums, "tile", 1), exchanged(far, "sub", 1)]
    else:
        mask = 1
        while mask < tiles:
            sums = sums + exchanged(sums, "tile", mask)
            mask *= 2
        parts = [sums]
    outputs = pl.pallas_call(
        update,
        out_shape=(jax.ShapeDtypeStruct(shape, F32),) * 3,
        in_specs=[WHOLE] * (len(parts) + 4),
        out_specs=(WHOLE,) * 3,
        compiler_params=limit(4),
        name="update",
    )(*[near(a) for a in (*parts, flat(increment), flat(residual), flat(direction), image)])
    return tuple(out.reshape(increment.shape) for out in outputs)


def solution(mesh):
    field = P(("member", "lev"), ("tile", "sub"), None)
    placed = (
        (field,) * 5
        + (P(),) * 5
        + (P(("tile", "sub")),) * 3
        + (P(("tile", "sub"), "lev", None), P())
    )
    return jax.shard_map(body, mesh=mesh, in_specs=placed, out_specs=(field,) * 3, check_vma=False)
```
